256 devices in a mesh: dp: 16 (over y, x_lo, core), mp: 16 (over x_hi, z).
Axes of the slice: x: 4 (x_hi: 2, x_lo: 2; x = x_hi * 2 + x_lo), y: 4, z: 8, core: 2. Of those that a mesh axis runs over, the one named last changes fastest.
Arguments:
- token_ids: int32 [32, 16], replicated, may hold values from 0 to 64511
- prompt_lengths: int32 [32], replicated, may hold values from 128 to 6144, as said below
- cache_codes: bfloat16 [32, 6144, 2, 1024], P('dp', 'mp'), may hold values from -1 to 1
- cache_scales: bfloat16 [32, 48, 2, 1024], P('dp', 'mp'), may hold values from 0.03 to 400
- embedding: bfloat16 [64512, 8192], P('mp', 'dp'), may hold values from -12 to 12
- norm_gain: bfloat16 [8192], P('dp'), may hold values from 0.099609375 to 1.8984375
- query_weight: bfloat16 [8192, 8192], P('dp', 'mp'), may hold values from -0.0625 to 0.0625
- key_value_weight: bfloat16 [8192, 2, 1024], P('dp'), may hold values from -0.0625 to 0.0625
- output_weight: bfloat16 [8192, 8192], P('mp', 'dp'), may hold values from -0.0625 to 0.0625
Outputs:
- layer_out: bfloat16 [32, 16, 8192], P(None, None, 'dp')
The draws below stay inside these ranges and needn't reach their ends.
Inputs may be any that keep to these rules, and one draw needn't show every extreme that they name: `prompt_lengths`: each a multiple of 128; some row has exactly 6144 in every draw.
All inputs are finite; a program needn't handle non-finite values.
Results may differ from the reference program's by a relative error of at most 0.0065.
The reference program's roundings to bfloat16 on the way (of `scaled`, `cache`, `weights` and `mixed`) count: a program that leaves them out, or rounds other values in their place, can miss the bound.
Values may be sent and summed in bfloat16 or wider, within the bound.
A program may use at most 128 MiB of HBM per device.

```python
import math
import jax
import jax.numpy as jnp
from jax import lax

D = 8192
QH = 64
KVH = 8
HEAD = 128
VOCAB = 64512
STORED_LENGTH = 6144
FACTOR_GROUP = 128
NEW = 16
QUESTION_COUNT = 32


def draw_prompt_lengths(key, part):
    first_key = jax.random.fold_in(key, 11)
    latter_entry_place = jax.random.fold_in(key, 12)
    blocks = jax.random.randint(first_key, (QUESTION_COUNT,), 1, STORED_LENGTH // FACTOR_GROUP + 1)
    longest = jax.random.randint(latter_entry_place, (), 0, QUESTION_COUNT)
    blocks = jnp.where(jnp.arange(QUESTION_COUNT) == longest, STORED_LENGTH // FACTOR_GROUP, blocks)
    return (blocks * FACTOR_GROUP).astype(jnp.int32)


def draw_cache_scales(key, part):
    first_key = jax.random.fold_in(key, 21)
    shape = (QUESTION_COUNT, STORED_LENGTH // FACTOR_GROUP, 2, KVH * HEAD)
    return jnp.exp(jax.random.uniform(first_key, shape, jnp.float32, math.log(0.03), math.log(3.0))).astype(jnp.bfloat16)


def draw_embedding(key, part):
    first_key = jax.random.fold_in(key, 31)
    latter_entry_place = jax.random.fold_in(key, 32)
    third_key = jax.random.fold_in(key, 33)
    beginning_shift = jnp.clip(jax.random.normal(first_key, (VOCAB, D), jnp.float32), -4.0, 4.0)
    row_scale = jnp.exp(jax.random.uniform(latter_entry_place, (VOCAB, 1), jnp.float32, math.log(0.1), 0.0))
    column_scale = jnp.exp(jax.random.uniform(third_key, (1, D), jnp.float32, math.log(0.3), math.log(3.0)))
    return (beginning_shift * row_scale * column_scale).astype(jnp.bfloat16)


def with_ends(drawn, key, least, largest):
    place = [jax.random.randint(jax.random.fold_in(key, axis), (), 0, length) for axis, length in enumerate(drawn.shape)]
    widest = drawn.shape.index(max(drawn.shape))
    next_to = place[:widest] + [(place[widest] + 1) % drawn.shape[widest]] + place[widest + 1:]
    return drawn.at[tuple(place)].set(least).at[tuple(next_to)].set(largest)


def block_scale(own_key, shape, pieces, low, high):
    def one(axis_at, shards_of):
        draws = jax.random.uniform(jax.random.fold_in(jax.random.fold_in(own_key, 6), axis_at), (shards_of,), jnp.float32, low / len(pieces), high / len(pieces))
        return jnp.repeat(jnp.exp(draws), shape[axis_at] // shards_of).reshape((-1,) + (1,) * (len(shape) - axis_at - 1))

    factor_of = one(*pieces[0])
    for cut in pieces[1:]:
        factor_of = factor_of * one(*cut)
    return factor_of


def centred(stream_key, extent, scale, limit, cuts=(), kind=jnp.bfloat16):
    entries = jax.random.normal(stream_key, extent, jnp.float32) * scale
    if len(cuts) > 0:
        entries = block_scale(stream_key, extent, cuts, -0.22, 0.18) * entries
    return jnp.clip(entries, min=-limit, max=limit).astype(kind)


def setup_inputs(seed: int = 0) -> dict:
    key_list = jax.random.split(jax.random.key(seed), 10)
    return {
        "token_ids": with_ends(jax.random.randint(key_list[0], (QUESTION_COUNT, NEW), 0, VOCAB), jax.random.fold_in(key_list[0], 1), 0, VOCAB - 1).astype(jnp.int32),
        "prompt_lengths": draw_prompt_lengths(jax.random.fold_in(key_list[9], 71), 0),
        "cache_codes": jnp.clip(jax.random.uniform(key_list[2], (QUESTION_COUNT, STORED_LENGTH, 2, KVH * HEAD), jnp.float32, -1.0, 1.0) * block_scale(key_list[2], (QUESTION_COUNT, STORED_LENGTH, 2, KVH * HEAD), ((0, 16), (1, 16)), -0.4, 0.0), -1.0, 1.0).astype(jnp.bfloat16),
        "cache_scales": draw_cache_scales(jax.random.fold_in(key_list[9], 71), 0),
        "embedding": draw_embedding(jax.random.fold_in(key_list[9], 71), 0),
        "norm_gain": jnp.clip(1.0 + 0.18 * jax.random.normal(key_list[5], (D,), jnp.float32), 0.099609375, 1.8984375).astype(jnp.bfloat16),
        "query_weight": centred(key_list[6], (D, QH * HEAD), D ** -0.5, 0.0625, ((0, 16), (1, 16))),
        "key_value_weight": centred(key_list[7], (D, 2, KVH * HEAD), D ** -0.5, 0.0625, ((0, 16),)),
        "output_weight": centred(key_list[8], (QH * HEAD, D), (QH * HEAD) ** -0.5, 0.0625, ((0, 16), (1, 16))),
    }


ROPE_BASE = 500000.0
EPSILON = 1e-05

def rotate(values, positions):
    width = values.shape[-1]
    half_width = width // 2
    exponent = jnp.arange(half_width, dtype=jnp.float32) * (2.0 / width)
    rates = jnp.exp(-jnp.log(ROPE_BASE) * exponent)
    angles = positions[..., None].astype(jnp.float32) * rates
    cosine = jnp.cos(angles)
    sinus_term = jnp.sin(angles)
    first = values[..., :half_width]
    second = values[..., half_width:]
    return jnp.concatenate([first * cosine - second * sinus_term, second * cosine + first * sinus_term], axis=-1)

def attend_row(queries, cache, new_keys, new_values, length):
    keys = jnp.concatenate([cache[:, 0], new_keys], axis=0).astype(jnp.float32)
    values = jnp.concatenate([cache[:, 1], new_values], axis=0).astype(jnp.float32)
    scores = jnp.einsum('tkgd,skd->kgts', queries.astype(jnp.float32), keys) * HEAD ** (-0.5)
    slots = jnp.arange(STORED_LENGTH + NEW, dtype=jnp.int32)
    steps = jnp.arange(NEW, dtype=jnp.int32)
    allowed = jnp.where(slots[None, :] < STORED_LENGTH, slots[None, :] < length, slots[None, :] - STORED_LENGTH <= steps[:, None])
    scores = jnp.where(allowed, scores, -jnp.inf)
    top = lax.optimization_barrier(jnp.max(scores, axis=-1, keepdims=True))
    lifted = jnp.exp(scores - top)
    weights = (lifted / lax.optimization_barrier(jnp.sum(lifted, axis=-1, keepdims=True))).astype(jnp.bfloat16)
    mixed = jnp.einsum('kgts,skd->tkgd', weights.astype(jnp.float32), values)
    return mixed.astype(jnp.bfloat16)

def reference(token_ids, prompt_lengths, cache_codes, cache_scales, embedding, norm_gain, query_weight, key_value_weight, output_weight):
    group = QH // KVH
    embedded = jnp.take(embedding, token_ids.reshape(-1), axis=0).astype(jnp.float32)
    scaled = (embedded * norm_gain.astype(jnp.float32)).astype(jnp.bfloat16)
    inverse = lax.rsqrt(lax.optimization_barrier(jnp.sum(embedded * embedded, axis=1)) / D + EPSILON)[:, None]
    queries = jnp.dot(scaled, query_weight, preferred_element_type=jnp.float32) * inverse
    fresh = jnp.dot(scaled, key_value_weight.reshape(D, 2 * KVH * HEAD), preferred_element_type=jnp.float32) * inverse
    positions = (prompt_lengths[:, None] + jnp.arange(NEW, dtype=jnp.int32)[None, :])[:, :, None]
    queries = rotate(queries.reshape(QUESTION_COUNT, NEW, QH, HEAD), positions).astype(jnp.bfloat16)
    queries = queries.reshape(QUESTION_COUNT, NEW, KVH, group, HEAD)
    fresh = fresh.reshape(QUESTION_COUNT, NEW, 2, KVH, HEAD)
    new_keys = rotate(fresh[:, :, 0], positions).astype(jnp.bfloat16)
    new_values = fresh[:, :, 1].astype(jnp.bfloat16)

    def one_row(items):
        codes, scales, query_row, key_row, value_row, length = items
        widened = codes.astype(jnp.float32).reshape(STORED_LENGTH // FACTOR_GROUP, FACTOR_GROUP, 2, KVH * HEAD)
        cache = (widened * scales.astype(jnp.float32)[:, None]).astype(jnp.bfloat16).reshape(STORED_LENGTH, 2, KVH, HEAD)
        return attend_row(query_row, cache, key_row, value_row, length)
    mixed = lax.map(one_row, (cache_codes, cache_scales, queries, new_keys, new_values, prompt_lengths))
    mixed = mixed.reshape(QUESTION_COUNT * NEW, QH * HEAD)
    result = jnp.dot(mixed, output_weight, preferred_element_type=jnp.float32)
    return result.astype(jnp.bfloat16).reshape(QUESTION_COUNT, NEW, D)
```

```python
import functools

import jax
import jax.numpy as jnp
from jax import lax
from jax.experimental import pallas as pl
from jax.experimental.pallas import tpu as pltpu
from jax.sharding import PartitionSpec as P

HEAD = 128
FACTOR_GROUP = 128
NEW = 16
ROPE_BASE = 500000.0
EPSILON = 1e-05
LOWEST = -1e30
MESH = pl.DeviceIdType.MESH
BF16 = jnp.bfloat16
F32 = jnp.float32

EMB_RS, EMB_AG, QKV_RS, QKV_AG, MIX_RS, STAT_RS, MIX_AG, OUT_RS, OUT_AG = range(9)


def dot(a, b):
    return jnp.dot(a, b, preferred_element_type=F32)


def dot_last(a, b):
    return lax.dot_general(a, b, (((1,), (1,)), ((), ())), preferred_element_type=F32)


def layer_kernel(
    nd, nm, width,
    lens_ref, ids_ref, table_ref, gain_ref, wkv_ref, scales_ref,
    codes_hbm, emb_hbm, wq_hbm, wo_hbm,
    out_hbm,
    emb, onehot, idsb, codes, wide, keys, valuesT, wq, wo,
    look, look_in, embedded, part, part_in, heads, mix, mix_in, stat, stat_in, mixed,
    outp, outp_in, final,
    send_sem, recv_sem, load_sem, store_sem,
):
    d, m = lax.axis_index("dp"), lax.axis_index("mp")
    groups = 2
    vocab = emb_hbm.shape[0]
    tokens = nd * NEW
    kvh = nm // 2
    span = codes_hbm.shape[1]
    blocks = span // FACTOR_GROUP
    lane = lambda shape: lax.broadcasted_iota(jnp.int32, shape, len(shape) - 1)

    def peer(axis, i):
        if axis == "mp":
            return (d, lax.rem(m + i, nm))
        return (lax.rem(d + i, nd), m)

    def me_of(axis):
        return (m, nm) if axis == "mp" else (d, nd)

    barrier = pltpu.get_barrier_semaphore()
    for axis in ("mp", "dp"):
        def hello(i, c, axis=axis):
            pl.semaphore_signal(barrier, inc=1, device_id=peer(axis, i), device_id_type=MESH)
            return c
        lax.fori_loop(1, me_of(axis)[1], hello, 0)

    chunk = vocab // 4
    loads = [
        pltpu.make_async_copy(
            emb_hbm.at[pl.ds(c * chunk, chunk)], emb.at[pl.ds(c * chunk, chunk)], load_sem.at[c]
        )
        for c in range(4)
    ]
    loads.append(pltpu.make_async_copy(wq_hbm, wq, load_sem.at[4]))
    loads.append(pltpu.make_async_copy(wo_hbm, wo, load_sem.at[5]))
    code_loads = [
        pltpu.make_async_copy(
            codes_hbm.at[g, :, :, pl.ds(k * HEAD, HEAD)], codes.at[g, k], load_sem.at[6 + g * kvh + k]
        )
        for g in range(groups)
        for k in range(kvh)
    ]
    for copy in loads + code_loads:
        copy.start()

    def scatter_copy(ph, g, axis, src, dst, i):
        me, n = me_of(axis)
        dest = lax.rem(me + i, n)
        return pltpu.make_async_remote_copy(
            src_ref=src.at[g, dest], dst_ref=dst.at[g, i - 1],
            send_sem=send_sem.at[0 if ph != STAT_RS else 1, g, i - 1],
            recv_sem=recv_sem.at[ph, g, i - 1],
            device_id=peer(axis, i), device_id_type=MESH,
        )

    def gather_copy(ph, g, axis, buf, i, at):
        return pltpu.make_async_remote_copy(
            src_ref=buf.at[g, at], dst_ref=buf.at[g, at],
            send_sem=send_sem.at[0, g, i - 1], recv_sem=recv_sem.at[ph, g, i - 1],
            device_id=peer(axis, i), device_id_type=MESH,
        )

    def scatter_start(ph, g, axis, src, dst):
        def go(i, c):
            scatter_copy(ph, g, axis, src, dst, i).start()
            return c
        lax.fori_loop(1, me_of(axis)[1], go, 0)

    def scatter_wait(ph, g, axis, src, dst):
        def go(i, c):
            scatter_copy(ph, g, axis, src, dst, i).wait()
            return c
        lax.fori_loop(1, me_of(axis)[1], go, 0)

    def gather_start(ph, g, axis, buf):
        me, n = me_of(axis)
        def go(i, c):
            gather_copy(ph, g, axis, buf, i, me).start()
            return c
        lax.fori_loop(1, n, go, 0)

    def gather_wait(ph, g, axis, buf):
        me, n = me_of(axis)
        def go(i, c):
            gather_copy(ph, g, axis, buf, i, me).wait_send()
            gather_copy(ph, g, axis, buf, i, lax.rem(me + n - i, n)).wait_recv()
            return c
        lax.fori_loop(1, n, go, 0)

    padded = emb.shape[0]
    if padded > vocab:
        emb[pl.ds(vocab, padded - vocab), :] = jnp.zeros((padded - vocab, emb.shape[1]), BF16)
    base = m * vocab

    def lookup(g):
        for j in range(nd):
            r = 2 * j + g
            idsb[pl.ds(j * NEW, NEW), :] = jnp.broadcast_to(ids_ref[:, r : r + 1] - base, (NEW, 128))

        def build(c, carry):
            for s in range(4):
                at = pl.multiple_of((c * 4 + s) * 128, 128)
                hit = idsb[...] - at == lane((tokens, 128))
                onehot[:, pl.ds(at, 128)] = jnp.where(hit, 1.0, 0.0).astype(BF16)
            return carry
        lax.fori_loop(0, padded // 512, build, 0)

    def look_dot(g):
        look[g] = dot(onehot[...], emb[...]).astype(BF16).reshape(nd, NEW, width)

    lookup(0)
    for c in range(4):
        loads[c].wait()
    look_dot(0)
    pl.semaphore_wait(barrier, nd + nm - 2)
    scatter_start(EMB_RS, 0, "mp", look, look_in)
    lookup(1)
    look_dot(1)
    scatter_start(EMB_RS, 1, "mp", look, look_in)

    def widen(g):
        def one(k, carry):
            wide[...] = codes[g, k].reshape(2 * span, HEAD).astype(F32)
            for b in range(blocks):
                sc = scales_ref[g, b, :, pl.ds(pl.multiple_of(k * HEAD, HEAD), HEAD)].astype(F32)
                rows = pl.ds(b * FACTOR_GROUP, FACTOR_GROUP)
                kk = wide[pl.ds(2 * b * FACTOR_GROUP, FACTOR_GROUP, 2), :] * sc[0:1]
                vv = wide[pl.ds(2 * b * FACTOR_GROUP + 1, FACTOR_GROUP, 2), :] * sc[1:2]
                keys[g, k, rows, :] = kk.astype(BF16)
                valuesT[g, k, :, rows] = vv.T.astype(BF16)
            return carry
        lax.fori_loop(0, kvh, one, 0)

    def emb_sum(g):
        scatter_wait(EMB_RS, g, "mp", look, look_in)
        total = look[g, m].astype(F32)
        for i in range(nm - 1):
            total = total + look_in[g, i].astype(F32)
        embedded[g, m] = total.astype(BF16)
        gather_start(EMB_AG, g, "mp", embedded)

    for copy in code_loads[:kvh]:
        copy.wait()
    widen(0)
    emb_sum(0)
    for copy in code_loads[kvh:]:
        copy.wait()
    emb_sum(1)
    widen(1)
    loads[4].wait()
    loads[5].wait()

    def project(g):
        gather_wait(EMB_AG, g, "mp", embedded)
        x = embedded[g].reshape(tokens, width).astype(F32)
        scaled = (x * gain_ref[...].astype(F32)).astype(BF16)
        square = x * x
        s = square[:, 0:128]
        for c in range(1, width // 128):
            s = s + square[:, c * 128 : (c + 1) * 128]
        s = s.reshape(nd, 2, 8, 128)
        a = s[:, 0].reshape(nd * 8, 128)
        b = s[:, 1].reshape(nd * 8, 128)
        a = a + pltpu.roll(a, 64, 1)
        b = b + pltpu.roll(b, 64, 1)
        part[g, :, 10] = jnp.where(lane(a.shape) < 64, a, b).reshape(nd, 8, 128)
        q = dot(scaled, wq[...])
        for c in range(4):
            part[g, :, 2 * c : 2 * c + 2] = q[:, c * HEAD : (c + 1) * HEAD].reshape(nd, 2, 8, 128)
        part[g, :, 8:10] = dot(scaled, wkv_ref[...]).reshape(nd, 2, 8, 128)
        scatter_start(QKV_RS, g, "dp", part, part_in)

    def rotate_heads(g):
        scatter_wait(QKV_RS, g, "dp", part, part_in)
        total = part[g, d]
        for i in range(nd - 1):
            total = total + part_in[g, i]
        sq = total[10]
        low = lane((8, 128)) < 64
        sums = jnp.concatenate(
            [
                jnp.sum(jnp.where(low, sq, 0.0), axis=1, keepdims=True),
                jnp.sum(jnp.where(low, 0.0, sq), axis=1, keepdims=True),
            ],
            axis=0,
        )
        inverse = lax.rsqrt(sums / (nd * width) + EPSILON)
        cosine, sine = table_ref[g, 0], table_ref[g, 1]
        odd = lax.rem(m, 2) == 1
        for c in range(5):
            v = total[2 * c : 2 * c + 2].reshape(NEW, HEAD) * inverse
            turned = v * cosine + pltpu.roll(v, 64, 1) * sine
            if c == 4:
                turned = jnp.where(odd, v, turned)
            heads[g, m, c] = turned.astype(BF16)
        gather_start(QKV_AG, g, "mp", heads)

    factor = HEAD ** (-0.5)
    half = lane((64, 128)) < 64
    half2 = lane((2, 128)) < 64

    def attend(g):
        gather_wait(QKV_AG, g, "mp", heads)
        live = lens_ref[2 * d + g] - m * span
        allowed = lax.broadcasted_iota(jnp.int32, (span, 128), 0) < live

        def one(k, carry):
            q = heads[g, pl.ds(2 * k, 2), 0:4].reshape(128, HEAD)
            s = jnp.where(allowed, dot_last(keys[g, k], q) * factor, -jnp.inf)
            top = jnp.maximum(jnp.max(s, axis=0, keepdims=True), LOWEST)
            p = jnp.exp(s - top)
            st = jnp.concatenate([top, jnp.sum(p, axis=0, keepdims=True)], axis=0)
            o = dot(valuesT[g, k], p.astype(BF16))
            lo, hi = o[0:64], o[64:128]
            mix[g, 2 * k] = jnp.where(half, lo, pltpu.roll(hi, 64, 1)).astype(BF16)
            mix[g, 2 * k + 1] = jnp.where(half, pltpu.roll(lo, 64, 1), hi).astype(BF16)
            turned = pltpu.roll(st, 64, 1)
            stat[g, 2 * k] = jnp.where(half2, st, turned)
            stat[g, 2 * k + 1] = jnp.where(half2, turned, st)
            return carry
        lax.fori_loop(0, kvh, one, 0)
        scatter_start(STAT_RS, g, "mp", stat, stat_in)
        scatter_start(MIX_RS, g, "mp", mix, mix_in)

    def fresh_part(g):
        pair = 2 * (m // 2)
        q = heads[g, m, 0:4].reshape(64, HEAD)
        q = jnp.concatenate([q, q], axis=0)
        s = dot_last(heads[g, pair, 4], q) * factor
        step = lax.rem(lane((NEW, 128)), NEW)
        s = jnp.where(lax.broadcasted_iota(jnp.int32, (NEW, 128), 0) <= step, s, -jnp.inf)
        top = jnp.max(s, axis=0, keepdims=True)
        p = jnp.exp(s - top)
        o = dot(heads[g, pair + 1, 4].astype(F32).T.astype(BF16), p.astype(BF16))
        return top, jnp.sum(p, axis=0, keepdims=True), jnp.where(half, o[0:64], o[64:128])

    def mix_heads(g):
        top_f, sum_f, o_f = fresh_part(g)
        scatter_wait(STAT_RS, g, "mp", stat, stat_in)
        scatter_wait(MIX_RS, g, "mp", mix, mix_in)
        stats = [stat[g, m]] + [stat_in[g, i] for i in range(nm - 1)]
        largest = top_f
        for st in stats:
            largest = jnp.maximum(largest, st[0:1])
        w = jnp.exp(top_f - largest)
        total = sum_f * w
        acc = o_f * w
        for i, st in enumerate(stats):
            w = jnp.exp(st[0:1] - largest)
            total = total + w * st[1:2]
            o = mix[g, m] if i == 0 else mix_in[g, i - 1]
            acc = acc + w * o.astype(F32)
        acc = acc / total
        full = jnp.concatenate([acc, pltpu.roll(acc, 64, 1)], axis=0)
        mixed[g, d] = full.T[0:64].astype(BF16).reshape(4, NEW, HEAD)
        gather_start(MIX_AG, g, "dp", mixed)

    def out_project(g):
        gather_wait(MIX_AG, g, "dp", mixed)
        a = jnp.concatenate([mixed[g, :, h].reshape(tokens, HEAD) for h in range(4)], axis=1)
        outp[g] = dot(a, wo[...]).astype(BF16).reshape(nd, NEW, width)
        scatter_start(OUT_RS, g, "mp", outp, outp_in)

    def out_sum(g):
        scatter_wait(OUT_RS, g, "mp", outp, outp_in)
        total = outp[g, m].astype(F32)
        for i in range(nm - 1):
            total = total + outp_in[g, i].astype(F32)
        final[g, m] = total.astype(BF16)
        gather_start(OUT_AG, g, "mp", final)

    def finish(g):
        gather_wait(OUT_AG, g, "mp", final)
        return pltpu.make_async_copy(final.at[g], out_hbm.at[:, g], store_sem.at[g])

    for stage in (project, rotate_heads, attend, mix_heads, out_project, out_sum):
        for g in range(groups):
            stage(g)
    stores = []
    for g in range(groups):
        copy = finish(g)
        copy.start()
        stores.append(copy)
    for copy in stores:
        copy.wait()


def on_device(
    token_ids, prompt_lengths, cache_codes, cache_scales, embedding, norm_gain,
    query_weight, key_value_weight, output_weight,
):
    nm, nd = lax.axis_size("mp"), lax.axis_size("dp")
    m, d = lax.axis_index("mp"), lax.axis_index("dp")
    vocab, width = embedding.shape
    rows, span = cache_codes.shape[:2]
    kvh = nm // 2
    padded = -(-vocab // 512) * 512
    tokens = nd * NEW

    wkv = lax.dynamic_slice(
        key_value_weight, (0, lax.rem(m, 2), (m // 2) * HEAD), (width, 1, HEAD)
    ).reshape(width, HEAD)
    lengths = lax.dynamic_slice_in_dim(prompt_lengths, d * rows, rows)
    positions = lengths[:, None] + jnp.arange(NEW, dtype=jnp.int32)[None, :]
    exponent = jnp.arange(HEAD // 2, dtype=F32) * (2.0 / HEAD)
    rates = jnp.exp(-jnp.log(ROPE_BASE) * exponent)
    angles = positions[..., None].astype(F32) * rates
    cosine, sine = jnp.cos(angles), jnp.sin(angles)
    table = jnp.stack(
        [
            jnp.concatenate([cosine, cosine], axis=-1),
            jnp.concatenate([-sine, sine], axis=-1),
        ],
        axis=1,
    )

    vmem = pl.BlockSpec(memory_space=pltpu.VMEM)
    hbm = pl.BlockSpec(memory_space=pl.ANY)
    smem = pl.BlockSpec(memory_space=pltpu.SMEM)
    V = pltpu.VMEM
    out = pl.pallas_call(
        functools.partial(layer_kernel, nd, nm, width),
        out_shape=jax.ShapeDtypeStruct((nd, rows, NEW, width), BF16),
        in_specs=[smem, vmem, vmem, vmem, vmem, vmem, hbm, hbm, hbm, hbm],
        out_specs=hbm,
        scratch_shapes=[
            V((padded, width), BF16),
            V((tokens, padded), BF16),
            V((tokens, 128), jnp.int32),
            V((rows, kvh, span, 2, HEAD), BF16),
            V((2 * span, HEAD), F32),
            V((rows, kvh, span, HEAD), BF16),
            V((rows, kvh, HEAD, span), BF16),
            V(query_weight.shape, BF16),
            V(output_weight.shape, BF16),
            V((rows, nd, NEW, width), BF16),
            V((rows, nm - 1, NEW, width), BF16),
            V((rows, nm, NEW, width), BF16),
            V((rows, nd, 11, 8, 128), F32),
            V((rows, nd - 1, 11, 8, 128), F32),
            V((rows, nm, 5, NEW, HEAD), BF16),
            V((rows, nm, 64, 128), BF16),
            V((rows, nm - 1, 64, 128), BF16),
            V((rows, nm, 2, 128), F32),
            V((rows, nm - 1, 2, 128), F32),
            V((rows, nd, 4, NEW, HEAD), BF16),
            V((rows, nd, NEW, width), BF16),
            V((rows, nm - 1, NEW, width), BF16),
            V((rows, nm, NEW, width), BF16),
            pltpu.SemaphoreType.DMA((2, rows, max(nm, nd) - 1)),
            pltpu.SemaphoreType.DMA((9, rows, max(nm, nd) - 1)),
            pltpu.SemaphoreType.DMA((6 + rows * kvh,)),
            pltpu.SemaphoreType.DMA((rows,)),
        ],
        compiler_params=pltpu.CompilerParams(
            collective_id=0, has_side_effects=True, vmem_limit_bytes=56 * 2**20
        ),
    )(
        prompt_lengths, token_ids.T, table, norm_gain.reshape(1, width), wkv, cache_scales,
        cache_codes, embedding, query_weight, output_weight,
    )
    return out.reshape(nd * rows, NEW, width)


def solution(mesh):
    return jax.shard_map(
        on_device,
        mesh=mesh,
        in_specs=(
            P(),
            P(),
            P("dp", "mp", None, None),
            P("dp", "mp", None, None),
            P("mp", "dp"),
            P("dp"),
            P("dp", "mp"),
            P("dp", None, None),
            P("mp", "dp"),
        ),
        out_specs=P(None, None, "dp"),
        check_vma=False,
    )
```

```python
import functools

import jax
import jax.numpy as jnp
from jax import lax
from jax.experimental import pallas as pl
from jax.experimental.pallas import tpu as pltpu
from jax.sharding import PartitionSpec as P

HEAD = 128
FACTOR_GROUP = 128
NEW = 16
ROPE_BASE = 500000.0
EPSILON = 1e-05
LOWEST = -1e30
MESH = pl.DeviceIdType.MESH
BF16 = jnp.bfloat16
F32 = jnp.float32

EMB_RS, EMB_AG, CORE_RS, QKV_RS, QKV_AG, KV_SWAP, MIX_RS, STAT_RS, MIX_AG, OUT_RS, OUT_AG = range(11)
SENDERS = {CORE_RS: 1, KV_SWAP: 1, STAT_RS: 2}


def dot(a, b):
    return jnp.dot(a, b, preferred_element_type=F32)


def dot_last(a, b):
    return lax.dot_general(a, b, (((1,), (1,)), ((), ())), preferred_element_type=F32)


def layer_kernel(
    nd, nm, width,
    lens_hbm, ids_hbm, gain_hbm, scales_hbm, codes_hbm, emb_hbm, wq_hbm, wkv_hbm, wo_hbm,
    out_hbm,
    emb, onehot, idsb, codes, wide, keys, valuesT, wq, wkv_in, wkv, wo,
    look, look_x, look_pair, look_in, embedded, part, part_core, part_sum, part_in, heads, fresh,
    mix, mix_in, stat, stat_in, mixed, outp, outp_x, outp_pair, outp_in, final,
    lens_ref, ids_ref, gain_ref, scales_ref,
    send_sem, recv_sem, load_sem, store_sem,
):
    d, m = lax.axis_index("dp"), lax.axis_index("mp")
    groups = 2
    vocab = emb_hbm.shape[0]
    tokens = nd * NEW
    kvh = nm // 2
    nz, nq = nm // 2, nd // 2
    column, z = m // nz, lax.rem(m, nz)
    chip, core = d // 2, lax.rem(d, 2)
    span = codes_hbm.shape[1]
    blocks = span // FACTOR_GROUP
    lane = lambda shape: lax.broadcasted_iota(jnp.int32, shape, len(shape) - 1)

    along_z = lambda i: (d, column * nz + lax.rem(z + i, nz))
    across = (d, (1 - column) * nz + z)
    along_mp = lambda i: (d, lax.rem(m + i, nm))
    along_dp = lambda i: (lax.rem(d + i, nd), m)
    along_chips = lambda i: (2 * lax.rem(chip + i, nq) + core, m)
    other_core = (2 * chip + 1 - core, m)
    kv_partner = (d, 2 * (m // 2) + 1 - lax.rem(m, 2))

    barrier = pltpu.get_barrier_semaphore()
    for along, n in ((along_mp, nm), (along_dp, nd)):
        def hello(i, c, along=along):
            pl.semaphore_signal(barrier, inc=1, device_id=along(i), device_id_type=MESH)
            return c
        lax.fori_loop(1, n, hello, 0)

    n_loads = 7 + groups * kvh
    small = [
        pltpu.make_async_copy(src, dst, load_sem.at[n_loads + i])
        for i, (src, dst) in enumerate(
            ((ids_hbm, ids_ref), (lens_hbm, lens_ref), (gain_hbm, gain_ref), (scales_hbm, scales_ref))
        )
    ]
    chunk = vocab // 4
    loads = [
        pltpu.make_async_copy(
            emb_hbm.at[pl.ds(c * chunk, chunk)], emb.at[pl.ds(c * chunk, chunk)], load_sem.at[c]
        )
        for c in range(4)
    ]
    loads.append(pltpu.make_async_copy(wq_hbm, wq, load_sem.at[4]))
    loads.append(pltpu.make_async_copy(wo_hbm, wo, load_sem.at[5]))
    loads.append(
        pltpu.make_async_copy(
            wkv_hbm.at[:, :, pl.ds(pl.multiple_of((m // 2) * HEAD, HEAD), HEAD)], wkv_in, load_sem.at[6]
        )
    )
    code_loads = [
        pltpu.make_async_copy(
            codes_hbm.at[g, :, :, pl.ds(k * HEAD, HEAD)], codes.at[g, k], load_sem.at[7 + g * kvh + k]
        )
        for g in range(groups)
        for k in range(kvh)
    ]
    for copy in small + loads + code_loads:
        copy.start()

    def remote(ph, g, k, src, dst, device):
        return pltpu.make_async_remote_copy(
            src_ref=src, dst_ref=dst,
            send_sem=send_sem.at[SENDERS.get(ph, 0), g, k], recv_sem=recv_sem.at[ph, g, k],
            device_id=device, device_id_type=MESH,
        )

    def loop(lo, hi, f):
        def body(i, c):
            f(i)
            return c
        lax.fori_loop(lo, hi, body, 0)

    def order(t):
        return nz // 2 + ((t + 1) // 2) * (1 - 2 * lax.rem(t, 2))

    def scatter_copy(ph, g, along, src, dst, dest, i):
        return remote(ph, g, i - 1, src.at[g, dest], dst.at[g, i - 1], along(i))

    def scatter_start(ph, g, along, src, dst, me, n):
        loop(1, n, lambda i: scatter_copy(ph, g, along, src, dst, lax.rem(me + i, n), i).start())

    def scatter_wait(ph, g, along, src, dst, me, n):
        loop(1, n, lambda i: scatter_copy(ph, g, along, src, dst, lax.rem(me + i, n), i).wait())

    def gather_start(ph, g, buf):
        loop(1, nd, lambda i: remote(ph, g, i - 1, buf.at[g, d], buf.at[g, d], along_dp(i)).start())

    def gather_wait(ph, g, buf):
        def go(i):
            remote(ph, g, i - 1, buf.at[g, d], buf.at[g, d], along_dp(i)).wait_send()
            at = lax.rem(d + nd - i, nd)
            remote(ph, g, i - 1, buf.at[g, at], buf.at[g, at], along_dp(i)).wait_recv()
        loop(1, nd, go)

    def z_copy(ph, g, buf, i, at):
        return remote(ph, g, i - 1, buf.at[g, at], buf.at[g, at], along_z(i))

    def x_copy(ph, g, buf, i, at):
        return remote(ph, g, nz - 1 + i, buf.at[g, at], buf.at[g, at], across)

    def behind(i):
        return lax.rem(z + nz - i, nz)

    def spread_start(ph, g, buf):
        loop(0, nz - 1, lambda t: z_copy(ph, g, buf, order(t), m).start())
        x_copy(ph, g, buf, 0, m).start()

    def spread_relay(ph, g, buf):
        def relay(t):
            i = order(t)
            at = column * nz + behind(i)
            z_copy(ph, g, buf, i, at).wait_recv()
            x_copy(ph, g, buf, i, at).start()
        loop(0, nz - 1, relay)

    def spread_wait(ph, g, buf):
        loop(1, nz, lambda i: z_copy(ph, g, buf, i, m).wait_send())
        def done(i):
            x_copy(ph, g, buf, i, column * nz + behind(i)).wait_send()
            x_copy(ph, g, buf, i, (1 - column) * nz + behind(i)).wait_recv()
        loop(0, nz, done)

    def ahead(i):
        return lax.rem(z + i, nz)

    def fold_x(ph, g, src, xin, i):
        return remote(ph, g, nz - 1 + i, src.at[g, (1 - column) * nz + ahead(i)], xin.at[g, i], across)

    def fold_z(ph, g, pair, zin, i):
        return remote(ph, g, i - 1, pair.at[g, i], zin.at[g, i - 1], along_z(i))

    def fold_start(ph, g, src, xin, zin):
        loop(0, nz - 1, lambda t: fold_x(ph, g, src, xin, order(t)).start())
        fold_x(ph, g, src, xin, 0).start()

    def fold_relay(ph, g, src, xin, pair, zin):
        def relay(t):
            i = order(t)
            fold_x(ph, g, src, xin, i).wait()
            pair[g, i] = (src[g, column * nz + ahead(i)].astype(F32) + xin[g, i].astype(F32)).astype(BF16)
            fold_z(ph, g, pair, zin, i).start()
        loop(0, nz - 1, relay)

    def fold_wait(ph, g, src, xin, pair, zin):
        total = src[g, m].astype(F32)
        fold_x(ph, g, src, xin, 0).wait()
        total = total + xin[g, 0].astype(F32)
        loop(1, nz, lambda i: fold_z(ph, g, pair, zin, i).wait())
        for i in range(nz - 1):
            total = total + zin[g, i].astype(F32)
        return total.astype(BF16)

    padded = emb.shape[0]
    if padded > vocab:
        emb[pl.ds(vocab, padded - vocab), :] = jnp.zeros((padded - vocab, emb.shape[1]), BF16)
    base = m * vocab

    def lookup(g):
        for j in range(nd):
            r = 2 * j + g
            idsb[pl.ds(j * NEW, NEW), :] = jnp.broadcast_to(ids_ref[:, r : r + 1] - base, (NEW, 128))

        def build(c, carry):
            for s in range(4):
                at = pl.multiple_of((c * 4 + s) * 128, 128)
                hit = idsb[...] - at == lane((tokens, 128))
                onehot[:, pl.ds(at, 128)] = jnp.where(hit, 1.0, 0.0).astype(BF16)
            return carry
        lax.fori_loop(0, padded // 512, build, 0)

    def look_dot(g):
        look[g] = dot(onehot[...], emb[...]).astype(BF16).reshape(nd, NEW, width)

    small[0].wait()
    lookup(0)
    for c in range(4):
        loads[c].wait()
    look_dot(0)
    pl.semaphore_wait(barrier, nd + nm - 2)
    fold_start(EMB_RS, 0, look, look_x, look_in)
    lookup(1)
    look_dot(1)
    fold_start(EMB_RS, 1, look, look_x, look_in)

    def widen(g):
        def one(k, carry):
            wide[pl.ds(0, 2 * span), :] = codes[g, k].reshape(2 * span, HEAD).astype(F32)
            for b in range(blocks):
                sc = scales_ref[g, b, :, pl.ds(pl.multiple_of(k * HEAD, HEAD), HEAD)].astype(F32)
                rows = pl.ds(b * FACTOR_GROUP, FACTOR_GROUP)
                kk = wide[pl.ds(2 * b * FACTOR_GROUP, FACTOR_GROUP, 2), :] * sc[0:1]
                vv = wide[pl.ds(2 * b * FACTOR_GROUP + 1, FACTOR_GROUP, 2), :] * sc[1:2]
                keys[g, k, rows, :] = kk.astype(BF16)
                valuesT[g, k, :, rows] = vv.T.astype(BF16)
            return carry
        lax.fori_loop(0, kvh, one, 0)

    def emb_sum(g):
        embedded[g, m] = fold_wait(EMB_RS, g, look, look_x, look_pair, look_in)
        spread_start(EMB_AG, g, embedded)

    for copy in small[1:] + code_loads[:kvh]:
        copy.wait()
    widen(0)
    def relays(f, *args):
        return lambda g: f(args[0], g, *args[1:])
    def staged(relay, stage):
        for f in (relay, stage):
            for g in range(groups):
                f(g)
    staged(relays(fold_relay, EMB_RS, look, look_x, look_pair, look_in), emb_sum)
    for copy in code_loads[kvh:]:
        copy.wait()
    widen(1)
    for copy in loads[4:]:
        copy.wait()
    wide[pl.ds(0, 2 * width), :] = wkv_in[...].reshape(2 * width, HEAD).astype(F32)
    odd = lax.rem(m, 2)
    wkv[...] = wide[pl.ds(odd, width, 2), :].astype(BF16)

    half_lane = lax.rem(lane((NEW, HEAD)), HEAD // 2)
    exponent = half_lane.astype(F32) * (2.0 / HEAD)
    rates = jnp.exp(-jnp.log(jnp.full((NEW, HEAD), ROPE_BASE, F32)) * exponent)
    steps = lax.broadcasted_iota(jnp.int32, (NEW, HEAD), 0)
    sign = jnp.where(lane((NEW, HEAD)) < HEAD // 2, -1.0, 1.0)
    tables = []
    for g in range(groups):
        angles = (lens_ref[2 * d + g] + steps).astype(F32) * rates
        tables.append((jnp.cos(angles), jnp.sin(angles) * sign))

    def project(g):
        spread_wait(EMB_AG, g, embedded)
        x = embedded[g].reshape(tokens, width).astype(F32)
        scaled = (x * gain_ref[...].astype(F32).reshape(1, width)).astype(BF16)
        square = x * x
        s = square[:, 0:128]
        for c in range(1, width // 128):
            s = s + square[:, c * 128 : (c + 1) * 128]
        s = s.reshape(nd, 2, 8, 128)
        a = s[:, 0].reshape(nd * 8, 128)
        b = s[:, 1].reshape(nd * 8, 128)
        a = a + pltpu.roll(a, 64, 1)
        b = b + pltpu.roll(b, 64, 1)
        s = jnp.where(lane(a.shape) < 64, a, b).reshape(nq, 2, 8, 128)
        q = dot(scaled, wq[...])
        kv = dot(scaled, wkv[...]).reshape(nq, 2, 2, 8, 128)
        q = [q[:, c * HEAD : (c + 1) * HEAD].reshape(nq, 2, 2, 8, 128) for c in range(4)] + [kv]
        for e in range(2):
            for c in range(5):
                part[g, e, :, 2 * c : 2 * c + 2] = q[c][:, e]
            part[g, e, :, 10] = s[:, e]
        core_copy(g).start()

    def core_copy(g):
        return remote(CORE_RS, g, 0, part.at[g, 1 - core], part_core.at[g], other_core)

    def join_cores(g):
        core_copy(g).wait()
        part_sum[g] = part[g, core] + part_core[g]
        scatter_start(QKV_RS, g, along_chips, part_sum, part_in, chip, nq)

    def kv_copy(g, at):
        return remote(KV_SWAP, g, 1, fresh.at[g, at], fresh.at[g, at], kv_partner)

    def rotate_heads(g):
        scatter_wait(QKV_RS, g, along_chips, part_sum, part_in, chip, nq)
        total = part_sum[g, chip]
        for i in range(nq - 1):
            total = total + part_in[g, i]
        sq = total[10]
        low = lane((8, 128)) < 64
        sums = jnp.concatenate(
            [
                jnp.sum(jnp.where(low, sq, 0.0), axis=1, keepdims=True),
                jnp.sum(jnp.where(low, 0.0, sq), axis=1, keepdims=True),
            ],
            axis=0,
        )
        inverse = lax.rsqrt(sums / (nd * width) + EPSILON)
        cosine, sine = tables[g]
        for c in range(5):
            v = total[2 * c : 2 * c + 2].reshape(NEW, HEAD) * inverse
            turned = v * cosine + pltpu.roll(v, 64, 1) * sine
            if c < 4:
                heads[g, m, c] = turned.astype(BF16)
            else:
                fresh[g, odd] = jnp.where(odd == 1, v, turned).astype(BF16)
        spread_start(QKV_AG, g, heads)
        kv_copy(g, odd).start()

    factor = HEAD ** (-0.5)
    half = lane((64, 128)) < 64
    half2 = lane((2, 128)) < 64

    def attend(g):
        spread_wait(QKV_AG, g, heads)
        live = lens_ref[2 * d + g] - m * span
        allowed = lax.broadcasted_iota(jnp.int32, (span, 128), 0) < live

        def one(k, carry):
            q = heads[g, pl.ds(2 * k, 2)].reshape(128, HEAD)
            s = jnp.where(allowed, dot_last(keys[g, k], q) * factor, -jnp.inf)
            top = jnp.maximum(jnp.max(s, axis=0, keepdims=True), LOWEST)
            p = jnp.exp(s - top)
            st = jnp.concatenate([top, jnp.sum(p, axis=0, keepdims=True)], axis=0)
            o = dot(valuesT[g, k], p.astype(BF16))
            lo, hi = o[0:64], o[64:128]
            mix[g, 2 * k] = jnp.where(half, lo, pltpu.roll(hi, 64, 1)).astype(BF16)
            mix[g, 2 * k + 1] = jnp.where(half, pltpu.roll(lo, 64, 1), hi).astype(BF16)
            turned = pltpu.roll(st, 64, 1)
            stat[g, 2 * k] = jnp.where(half2, st, turned)
            stat[g, 2 * k + 1] = jnp.where(half2, turned, st)
            return carry
        lax.fori_loop(0, kvh, one, 0)
        scatter_start(STAT_RS, g, along_mp, stat, stat_in, m, nm)
        scatter_start(MIX_RS, g, along_mp, mix, mix_in, m, nm)

    def fresh_part(g):
        kv_copy(g, odd).wait_send()
        kv_copy(g, 1 - odd).wait_recv()
        q = heads[g, m].reshape(64, HEAD)
        q = jnp.concatenate([q, q], axis=0)
        s = dot_last(fresh[g, 0], q) * factor
        step = lax.rem(lane((NEW, 128)), NEW)
        s = jnp.where(lax.broadcasted_iota(jnp.int32, (NEW, 128), 0) <= step, s, -jnp.inf)
        top = jnp.max(s, axis=0, keepdims=True)
        p = jnp.exp(s - top)
        o = dot(fresh[g, 1].astype(F32).T.astype(BF16), p.astype(BF16))
        return top, jnp.sum(p, axis=0, keepdims=True), jnp.where(half, o[0:64], o[64:128])

    def mix_heads(g):
        top_f, sum_f, o_f = fresh_part(g)
        scatter_wait(STAT_RS, g, along_mp, stat, stat_in, m, nm)
        scatter_wait(MIX_RS, g, along_mp, mix, mix_in, m, nm)
        stats = [stat[g, m]] + [stat_in[g, i] for i in range(nm - 1)]
        largest = top_f
        for st in stats:
            largest = jnp.maximum(largest, st[0:1])
        w = jnp.exp(top_f - largest)
        total = sum_f * w
        acc = o_f * w
        for i, st in enumerate(stats):
            w = jnp.exp(st[0:1] - largest)
            total = total + w * st[1:2]
            o = mix[g, m] if i == 0 else mix_in[g, i - 1]
            acc = acc + w * o.astype(F32)
        acc = acc / total
        full = jnp.concatenate([acc, pltpu.roll(acc, 64, 1)], axis=0)
        mixed[g, d] = full.T[0:64].astype(BF16).reshape(4, NEW, HEAD)
        gather_start(MIX_AG, g, mixed)

    def out_project(g):
        gather_wait(MIX_AG, g, mixed)
        a = jnp.concatenate([mixed[g, :, h].reshape(tokens, HEAD) for h in range(4)], axis=1)
        outp[g] = dot(a, wo[...]).astype(BF16).reshape(nd, NEW, width)
        fold_start(OUT_RS, g, outp, outp_x, outp_in)

    def out_sum(g):
        final[g, m] = fold_wait(OUT_RS, g, outp, outp_x, outp_pair, outp_in)
        spread_start(OUT_AG, g, final)

    def finish(g):
        spread_wait(OUT_AG, g, final)
        return pltpu.make_async_copy(final.at[g], out_hbm.at[:, g], store_sem.at[g])

    nothing = lambda g: None
    staged(relays(spread_relay, EMB_AG, embedded), project)
    staged(nothing, join_cores)
    staged(nothing, rotate_heads)
    staged(relays(spread_relay, QKV_AG, heads), attend)
    staged(nothing, mix_heads)
    staged(nothing, out_project)
    staged(relays(fold_relay, OUT_RS, outp, outp_x, outp_pair, outp_in), out_sum)
    spread_relay(OUT_AG, 0, final)
    spread_relay(OUT_AG, 1, final)
    stores = []
    for g in range(groups):
        copy = finish(g)
        copy.start()
        stores.append(copy)
    for copy in stores:
        copy.wait()


def on_device(
    token_ids, prompt_lengths, cache_codes, cache_scales, embedding, norm_gain,
    query_weight, key_value_weight, output_weight,
):
    nm, nd = lax.axis_size("mp"), lax.axis_size("dp")
    vocab, width = embedding.shape
    rows, span = cache_codes.shape[:2]
    kvh = nm // 2
    nz, nq = nm // 2, nd // 2
    padded = -(-vocab // 512) * 512
    tokens = nd * NEW

    hbm = pl.BlockSpec(memory_space=pltpu.HBM)
    V = pltpu.VMEM
    out = pl.pallas_call(
        functools.partial(layer_kernel, nd, nm, width),
        out_shape=jax.ShapeDtypeStruct((nd, rows, NEW, width), BF16),
        in_specs=[hbm] * 9,
        out_specs=pl.BlockSpec(memory_space=pl.ANY),
        scratch_shapes=[
            V((padded, width), BF16),
            V((tokens, padded), BF16),
            V((tokens, 128), jnp.int32),
            V((rows, kvh, span, 2, HEAD), BF16),
            V((2 * max(span, width), HEAD), F32),
            V((rows, kvh, span, HEAD), BF16),
            V((rows, kvh, HEAD, span), BF16),
            V(query_weight.shape, BF16),
            V((width, 2, HEAD), BF16),
            V((width, HEAD), BF16),
            V(output_weight.shape, BF16),
            V((rows, nd, NEW, width), BF16),
            V((rows, nz, NEW, width), BF16),
            V((rows, nz, NEW, width), BF16),
            V((rows, nz - 1, NEW, width), BF16),
            V((rows, nm, NEW, width), BF16),
            V((rows, 2, nq, 11, 8, 128), F32),
            V((rows, nq, 11, 8, 128), F32),
            V((rows, nq, 11, 8, 128), F32),
            V((rows, nq - 1, 11, 8, 128), F32),
            V((rows, nm, 4, NEW, HEAD), BF16),
            V((rows, 2, NEW, HEAD), BF16),
            V((rows, nm, 64, 128), BF16),
            V((rows, nm - 1, 64, 128), BF16),
            V((rows, nm, 2, 128), F32),
            V((rows, nm - 1, 2, 128), F32),
            V((rows, nd, 4, NEW, HEAD), BF16),
            V((rows, nd, NEW, width), BF16),
            V((rows, nz, NEW, width), BF16),
            V((rows, nz, NEW, width), BF16),
            V((rows, nz - 1, NEW, width), BF16),
            V((rows, nm, NEW, width), BF16),
            pltpu.SMEM(prompt_lengths.shape, jnp.int32),
            V((NEW, rows * nd), jnp.int32),
            V(norm_gain.shape, BF16),
            V(cache_scales.shape, BF16),
            pltpu.SemaphoreType.DMA((3, rows, max(nm, nd) - 1)),
            pltpu.SemaphoreType.DMA((11, rows, max(nm, nd) - 1)),
            pltpu.SemaphoreType.DMA((11 + rows * kvh,)),
            pltpu.SemaphoreType.DMA((rows,)),
        ],
        compiler_params=pltpu.CompilerParams(
            collective_id=0, has_side_effects=True, vmem_limit_bytes=56 * 2**20
        ),
    )(
        prompt_lengths, token_ids.T, norm_gain, cache_scales,
        cache_codes, embedding, query_weight, key_value_weight, output_weight,
    )
    return out.reshape(nd * rows, NEW, width)


def solution(mesh):
    return jax.shard_map(
        on_device,
        mesh=mesh,
        in_specs=(
            P(),
            P(),
            P("dp", "mp", None, None),
            P("dp", "mp", None, None),
            P("mp", "dp"),
            P("dp"),
            P("dp", "mp"),
            P("dp", None, None),
            P("mp", "dp"),
        ),
        out_specs=P(None, None, "dp"),
        check_vma=False,
    )
```

```python
import functools

import jax
import jax.numpy as jnp
from jax import lax
from jax.experimental import pallas as pl
from jax.experimental.pallas import tpu as pltpu
from jax.sharding import PartitionSpec as P

HEAD = 128
FACTOR_GROUP = 128
NEW = 16
ROPE_BASE = 500000.0
EPSILON = 1e-05
LOWEST = -1e30
MESH = pl.DeviceIdType.MESH
BF16 = jnp.bfloat16
F32 = jnp.float32

EMB_RS, EMB_AG, CORE_RS, QKV_RS, QKV_AG, KV_SWAP, MIX_RS, STAT_RS, MIX_AG, OUT_RS, OUT_AG = range(11)
SENDERS = {CORE_RS: 1, KV_SWAP: 1, STAT_RS: 2}


def dot(a, b):
    return jnp.dot(a, b, preferred_element_type=F32)


def dot_last(a, b):
    return lax.dot_general(a, b, (((1,), (1,)), ((), ())), preferred_element_type=F32)


def layer_kernel(
    nd, nm, width,
    lens_hbm, ids_hbm, gain_hbm, scales_hbm, codes_hbm, emb_hbm, wq_hbm, wkv_hbm, wo_hbm,
    out_hbm,
    emb, onehot, idsb, codes, wide, keys, valuesT, wq, wkv_in, wkv, wo,
    look, look_x, look_pair, look_in, embedded, part, part_core, part_sum, part_in, heads, fresh,
    mix, mix_x, mix_pair, mix_in, stat, stat_x, stat_pair, stat_in, mixed, outp, outp_x, outp_pair, outp_in, final,
    lens_ref, ids_ref, gain_ref, scales_ref,
    send_sem, recv_sem, load_sem, store_sem,
):
    d, m = lax.axis_index("dp"), lax.axis_index("mp")
    groups = 2
    vocab = emb_hbm.shape[0]
    tokens = nd * NEW
    kvh = nm // 2
    nz, nq = nm // 2, nd // 2
    column, z = m // nz, lax.rem(m, nz)
    chip, core = d // 2, lax.rem(d, 2)
    span = codes_hbm.shape[1]
    blocks = span // FACTOR_GROUP
    lane = lambda shape: lax.broadcasted_iota(jnp.int32, shape, len(shape) - 1)

    along_z = lambda i: (d, column * nz + lax.rem(z + i, nz))
    across = (d, (1 - column) * nz + z)
    along_dp = lambda i: (lax.rem(d + i, nd), m)
    along_chips = lambda i: (2 * lax.rem(chip + i, nq) + core, m)
    other_core = (2 * chip + 1 - core, m)
    kv_partner = (d, 2 * (m // 2) + 1 - lax.rem(m, 2))

    barrier = pltpu.get_barrier_semaphore()
    pl.semaphore_signal(barrier, inc=1, device_id=across, device_id_type=MESH)
    for along, n in ((along_z, nz), (along_dp, nd)):
        def hello(i, c, along=along):
            pl.semaphore_signal(barrier, inc=1, device_id=along(i), device_id_type=MESH)
            return c
        lax.fori_loop(1, n, hello, 0)

    n_loads = 7 + groups * kvh
    small = [
        pltpu.make_async_copy(src, dst, load_sem.at[n_loads + i])
        for i, (src, dst) in enumerate(
            ((ids_hbm, ids_ref), (lens_hbm, lens_ref), (gain_hbm, gain_ref), (scales_hbm, scales_ref))
        )
    ]
    chunk = vocab // 4
    loads = [
        pltpu.make_async_copy(
            emb_hbm.at[pl.ds(c * chunk, chunk)], emb.at[pl.ds(c * chunk, chunk)], load_sem.at[c]
        )
        for c in range(4)
    ]
    loads.append(pltpu.make_async_copy(wq_hbm, wq, load_sem.at[4]))
    loads.append(pltpu.make_async_copy(wo_hbm, wo, load_sem.at[5]))
    loads.append(
        pltpu.make_async_copy(
            wkv_hbm.at[:, :, pl.ds(pl.multiple_of((m // 2) * HEAD, HEAD), HEAD)], wkv_in, load_sem.at[6]
        )
    )
    code_loads = [
        pltpu.make_async_copy(
            codes_hbm.at[g, :, :, pl.ds(k * HEAD, HEAD)], codes.at[g, k], load_sem.at[7 + g * kvh + k]
        )
        for g in range(groups)
        for k in range(kvh)
    ]
    for copy in small + loads + code_loads:
        copy.start()

    def remote(ph, g, k, src, dst, device):
        return pltpu.make_async_remote_copy(
            src_ref=src, dst_ref=dst,
            send_sem=send_sem.at[SENDERS.get(ph, 0), g, k], recv_sem=recv_sem.at[ph, g, k],
            device_id=device, device_id_type=MESH,
        )

    def loop(lo, hi, f):
        def body(i, c):
            f(i)
            return c
        lax.fori_loop(lo, hi, body, 0)

    def order(t):
        return nz // 2 + ((t + 1) // 2) * (1 - 2 * lax.rem(t, 2))

    def scatter_copy(ph, g, along, src, dst, dest, i):
        return remote(ph, g, i - 1, src.at[g, dest], dst.at[g, i - 1], along(i))

    def scatter_start(ph, g, along, src, dst, me, n):
        loop(1, n, lambda i: scatter_copy(ph, g, along, src, dst, lax.rem(me + i, n), i).start())

    def scatter_wait(ph, g, along, src, dst, me, n):
        loop(1, n, lambda i: scatter_copy(ph, g, along, src, dst, lax.rem(me + i, n), i).wait())

    def gather_start(ph, g, buf):
        loop(1, nd, lambda i: remote(ph, g, i - 1, buf.at[g, d], buf.at[g, d], along_dp(i)).start())

    def gather_wait(ph, g, buf):
        def go(i):
            remote(ph, g, i - 1, buf.at[g, d], buf.at[g, d], along_dp(i)).wait_send()
            at = lax.rem(d + nd - i, nd)
            remote(ph, g, i - 1, buf.at[g, at], buf.at[g, at], along_dp(i)).wait_recv()
        loop(1, nd, go)

    def z_copy(ph, g, buf, i, at):
        return remote(ph, g, i - 1, buf.at[g, at], buf.at[g, at], along_z(i))

    def x_copy(ph, g, buf, i, at):
        return remote(ph, g, nz - 1 + i, buf.at[g, at], buf.at[g, at], across)

    def behind(i):
        return lax.rem(z + nz - i, nz)

    def spread_start(ph, g, buf):
        loop(0, nz - 1, lambda t: z_copy(ph, g, buf, order(t), m).start())
        x_copy(ph, g, buf, 0, m).start()

    def spread_relay(ph, g, buf):
        def relay(t):
            i = order(t)
            at = column * nz + behind(i)
            z_copy(ph, g, buf, i, at).wait_recv()
            x_copy(ph, g, buf, i, at).start()
        loop(0, nz - 1, relay)

    def spread_wait(ph, g, buf):
        loop(1, nz, lambda i: z_copy(ph, g, buf, i, m).wait_send())
        def done(i):
            x_copy(ph, g, buf, i, column * nz + behind(i)).wait_send()
            x_copy(ph, g, buf, i, (1 - column) * nz + behind(i)).wait_recv()
        loop(0, nz, done)

    def ahead(i):
        return lax.rem(z + i, nz)

    def fold_x(ph, g, src, xin, i):
        return remote(ph, g, nz - 1 + i, src.at[g, (1 - column) * nz + ahead(i)], xin.at[g, i], across)

    def fold_z(ph, g, pair, zin, i):
        return remote(ph, g, i - 1, pair.at[g, i], zin.at[g, i - 1], along_z(i))

    def fold_start(ph, g, src, xin, zin):
        loop(0, nz - 1, lambda t: fold_x(ph, g, src, xin, order(t)).start())
        fold_x(ph, g, src, xin, 0).start()

    def fold_relay(ph, g, src, xin, pair, zin):
        def relay(t):
            i = order(t)
            fold_x(ph, g, src, xin, i).wait()
            pair[g, i] = (src[g, column * nz + ahead(i)].astype(F32) + xin[g, i].astype(F32)).astype(BF16)
            fold_z(ph, g, pair, zin, i).start()
        loop(0, nz - 1, relay)

    def fold_wait(ph, g, src, xin, pair, zin):
        total = src[g, m].astype(F32)
        fold_x(ph, g, src, xin, 0).wait()
        total = total + xin[g, 0].astype(F32)
        loop(1, nz, lambda i: fold_z(ph, g, pair, zin, i).wait())
        for i in range(nz - 1):
            total = total + zin[g, i].astype(F32)
        return total.astype(BF16)

    padded = emb.shape[0]
    if padded > vocab:
        emb[pl.ds(vocab, padded - vocab), :] = jnp.zeros((padded - vocab, emb.shape[1]), BF16)
    base = m * vocab

    def lookup(g):
        for j in range(nd):
            r = 2 * j + g
            idsb[pl.ds(j * NEW, NEW), :] = jnp.broadcast_to(ids_ref[:, r : r + 1] - base, (NEW, 128))

        def build(c, carry):
            for s in range(4):
                at = pl.multiple_of((c * 4 + s) * 128, 128)
                hit = idsb[...] - at == lane((tokens, 128))
                onehot[:, pl.ds(at, 128)] = jnp.where(hit, 1.0, 0.0).astype(BF16)
            return carry
        lax.fori_loop(0, padded // 512, build, 0)

    def look_dot(g):
        look[g] = dot(onehot[...], emb[...]).astype(BF16).reshape(nd, NEW, width)

    small[0].wait()
    lookup(0)
    for c in range(4):
        loads[c].wait()
    look_dot(0)
    pl.semaphore_wait(barrier, nd + nz - 1)
    fold_start(EMB_RS, 0, look, look_x, look_in)
    lookup(1)
    look_dot(1)
    fold_start(EMB_RS, 1, look, look_x, look_in)

    def widen(g):
        def one(k, carry):
            wide[pl.ds(0, 2 * span), :] = codes[g, k].reshape(2 * span, HEAD).astype(F32)
            for b in range(blocks):
                sc = scales_ref[g, b, :, pl.ds(pl.multiple_of(k * HEAD, HEAD), HEAD)].astype(F32)
                rows = pl.ds(b * FACTOR_GROUP, FACTOR_GROUP)
                kk = wide[pl.ds(2 * b * FACTOR_GROUP, FACTOR_GROUP, 2), :] * sc[0:1]
                vv = wide[pl.ds(2 * b * FACTOR_GROUP + 1, FACTOR_GROUP, 2), :] * sc[1:2]
                keys[g, k, rows, :] = kk.astype(BF16)
                valuesT[g, k, :, rows] = vv.T.astype(BF16)
            return carry
        lax.fori_loop(0, kvh, one, 0)

    def emb_sum(g):
        embedded[g, m] = fold_wait(EMB_RS, g, look, look_x, look_pair, look_in)
        spread_start(EMB_AG, g, embedded)

    for copy in small[1:] + code_loads[:kvh]:
        copy.wait()
    widen(0)
    def relays(f, *args):
        return lambda g: f(args[0], g, *args[1:])
    def staged(relay, stage):
        for f in (relay, stage):
            for g in range(groups):
                f(g)
    staged(relays(fold_relay, EMB_RS, look, look_x, look_pair, look_in), emb_sum)
    for copy in code_loads[kvh:]:
        copy.wait()
    widen(1)
    for copy in loads[4:]:
        copy.wait()
    wide[pl.ds(0, 2 * width), :] = wkv_in[...].reshape(2 * width, HEAD).astype(F32)
    odd = lax.rem(m, 2)
    wkv[...] = wide[pl.ds(odd, width, 2), :].astype(BF16)

    half_lane = lax.rem(lane((NEW, HEAD)), HEAD // 2)
    exponent = half_lane.astype(F32) * (2.0 / HEAD)
    rates = jnp.exp(-jnp.log(jnp.full((NEW, HEAD), ROPE_BASE, F32)) * exponent)
    steps = lax.broadcasted_iota(jnp.int32, (NEW, HEAD), 0)
    sign = jnp.where(lane((NEW, HEAD)) < HEAD // 2, -1.0, 1.0)
    tables = []
    for g in range(groups):
        angles = (lens_ref[2 * d + g] + steps).astype(F32) * rates
        tables.append((jnp.cos(angles), jnp.sin(angles) * sign))

    def project(g):
        spread_wait(EMB_AG, g, embedded)
        x = embedded[g].reshape(tokens, width).astype(F32)
        scaled = (x * gain_ref[...].astype(F32).reshape(1, width)).astype(BF16)
        square = x * x
        s = square[:, 0:128]
        for c in range(1, width // 128):
            s = s + square[:, c * 128 : (c + 1) * 128]
        s = s.reshape(nd, 2, 8, 128)
        a = s[:, 0].reshape(nd * 8, 128)
        b = s[:, 1].reshape(nd * 8, 128)
        a = a + pltpu.roll(a, 64, 1)
        b = b + pltpu.roll(b, 64, 1)
        s = jnp.where(lane(a.shape) < 64, a, b).reshape(nq, 2, 8, 128)
        q = dot(scaled, wq[...])
        kv = dot(scaled, wkv[...]).reshape(nq, 2, 2, 8, 128)
        q = [q[:, c * HEAD : (c + 1) * HEAD].reshape(nq, 2, 2, 8, 128) for c in range(4)] + [kv]
        for e in range(2):
            for c in range(5):
                part[g, e, :, 2 * c : 2 * c + 2] = q[c][:, e]
            part[g, e, :, 10] = s[:, e]
        core_copy(g).start()

    def core_copy(g):
        return remote(CORE_RS, g, 0, part.at[g, 1 - core], part_core.at[g], other_core)

    def join_cores(g):
        core_copy(g).wait()
        part_sum[g] = part[g, core] + part_core[g]
        scatter_start(QKV_RS, g, along_chips, part_sum, part_in, chip, nq)

    def kv_copy(g, at):
        return remote(KV_SWAP, g, 1, fresh.at[g, at], fresh.at[g, at], kv_partner)

    def rotate_heads(g):
        scatter_wait(QKV_RS, g, along_chips, part_sum, part_in, chip, nq)
        total = part_sum[g, chip]
        for i in range(nq - 1):
            total = total + part_in[g, i]
        sq = total[10]
        low = lane((8, 128)) < 64
        sums = jnp.concatenate(
            [
                jnp.sum(jnp.where(low, sq, 0.0), axis=1, keepdims=True),
                jnp.sum(jnp.where(low, 0.0, sq), axis=1, keepdims=True),
            ],
            axis=0,
        )
        inverse = lax.rsqrt(sums / (nd * width) + EPSILON)
        cosine, sine = tables[g]
        for c in range(5):
            v = total[2 * c : 2 * c + 2].reshape(NEW, HEAD) * inverse
            turned = v * cosine + pltpu.roll(v, 64, 1) * sine
            if c < 4:
                heads[g, m, c] = turned.astype(BF16)
            else:
                fresh[g, odd] = jnp.where(odd == 1, v, turned).astype(BF16)
        spread_start(QKV_AG, g, heads)
        kv_copy(g, odd).start()

    factor = HEAD ** (-0.5)
    half = lane((64, 128)) < 64
    half2 = lane((2, 128)) < 64

    def attend(g):
        spread_wait(QKV_AG, g, heads)
        live = lens_ref[2 * d + g] - m * span
        allowed = lax.broadcasted_iota(jnp.int32, (span, 128), 0) < live

        def one(k, carry):
            q = heads[g, pl.ds(2 * k, 2)].reshape(128, HEAD)
            s = jnp.where(allowed, dot_last(keys[g, k], q) * factor, -jnp.inf)
            top = jnp.maximum(jnp.max(s, axis=0, keepdims=True), LOWEST)
            p = jnp.exp(s - top)
            st = jnp.concatenate([top, jnp.sum(p, axis=0, keepdims=True)], axis=0)
            o = dot(valuesT[g, k], p.astype(BF16))
            lo, hi = o[0:64], o[64:128]
            mix[g, 2 * k] = jnp.where(half, lo, pltpu.roll(hi, 64, 1)).astype(BF16)
            mix[g, 2 * k + 1] = jnp.where(half, pltpu.roll(lo, 64, 1), hi).astype(BF16)
            turned = pltpu.roll(st, 64, 1)
            stat[g, 2 * k] = jnp.where(half2, st, turned)
            stat[g, 2 * k + 1] = jnp.where(half2, turned, st)
            return carry
        lax.fori_loop(0, kvh, one, 0, unroll=True)
        def go(i):
            merge_x(g, i, MIX_RS).start()
            merge_x(g, i, STAT_RS).start()
        loop(0, nz - 1, lambda t: go(order(t)))
        go(0)

    def merge_x(g, i, ph):
        src, dst = (mix, mix_x) if ph == MIX_RS else (stat, stat_x)
        return fold_x(ph, g, src, dst, i)

    def merge_z(g, i, ph):
        src, dst = (mix_pair, mix_in) if ph == MIX_RS else (stat_pair, stat_in)
        return fold_z(ph, g, src, dst, i)

    def merge(g, i):
        merge_x(g, i, STAT_RS).wait()
        merge_x(g, i, MIX_RS).wait()
        at = column * nz + ahead(i)
        a, b = stat[g, at], stat_x[g, i]
        top = jnp.maximum(a[0:1], b[0:1])
        wa, wb = jnp.exp(a[0:1] - top), jnp.exp(b[0:1] - top)
        stat_pair[g, i] = jnp.concatenate([top, wa * a[1:2] + wb * b[1:2]], axis=0)
        mix_pair[g, i] = (wa * mix[g, at].astype(F32) + wb * mix_x[g, i].astype(F32)).astype(BF16)

    def merge_relay(g):
        def relay(t):
            i = order(t)
            merge(g, i)
            merge_z(g, i, MIX_RS).start()
            merge_z(g, i, STAT_RS).start()
        loop(0, nz - 1, relay)
        merge(g, 0)

    def fresh_part(g):
        kv_copy(g, odd).wait_send()
        kv_copy(g, 1 - odd).wait_recv()
        q = heads[g, m].reshape(64, HEAD)
        q = jnp.concatenate([q, q], axis=0)
        s = dot_last(fresh[g, 0], q) * factor
        step = lax.rem(lane((NEW, 128)), NEW)
        s = jnp.where(lax.broadcasted_iota(jnp.int32, (NEW, 128), 0) <= step, s, -jnp.inf)
        top = jnp.max(s, axis=0, keepdims=True)
        p = jnp.exp(s - top)
        o = dot(fresh[g, 1].astype(F32).T.astype(BF16), p.astype(BF16))
        return top, jnp.sum(p, axis=0, keepdims=True), jnp.where(half, o[0:64], o[64:128])

    def mix_heads(g):
        top_f, sum_f, o_f = fresh_part(g)
        def done(i):
            merge_z(g, i, STAT_RS).wait()
            merge_z(g, i, MIX_RS).wait()
        loop(1, nz, done)
        stats = [stat_pair[g, 0]] + [stat_in[g, i] for i in range(nz - 1)]
        largest = top_f
        for st in stats:
            largest = jnp.maximum(largest, st[0:1])
        w = jnp.exp(top_f - largest)
        total = sum_f * w
        acc = o_f * w
        for i, st in enumerate(stats):
            w = jnp.exp(st[0:1] - largest)
            total = total + w * st[1:2]
            o = mix_pair[g, 0] if i == 0 else mix_in[g, i - 1]
            acc = acc + w * o.astype(F32)
        acc = acc / total
        full = jnp.concatenate([acc, pltpu.roll(acc, 64, 1)], axis=0)
        mixed[g, d] = full.T[0:64].astype(BF16).reshape(4, NEW, HEAD)
        gather_start(MIX_AG, g, mixed)

    def out_project(g):
        gather_wait(MIX_AG, g, mixed)
        a = jnp.concatenate([mixed[g, :, h].reshape(tokens, HEAD) for h in range(4)], axis=1)
        outp[g] = dot(a, wo[...]).astype(BF16).reshape(nd, NEW, width)
        fold_start(OUT_RS, g, outp, outp_x, outp_in)

    def out_sum(g):
        final[g, m] = fold_wait(OUT_RS, g, outp, outp_x, outp_pair, outp_in)
        spread_start(OUT_AG, g, final)

    def finish(g):
        spread_wait(OUT_AG, g, final)
        return pltpu.make_async_copy(final.at[g], out_hbm.at[:, g], store_sem.at[g])

    nothing = lambda g: None
    staged(relays(spread_relay, EMB_AG, embedded), project)
    staged(nothing, join_cores)
    staged(nothing, rotate_heads)
    staged(relays(spread_relay, QKV_AG, heads), attend)
    staged(merge_relay, mix_heads)
    staged(nothing, out_project)
    staged(relays(fold_relay, OUT_RS, outp, outp_x, outp_pair, outp_in), out_sum)
    spread_relay(OUT_AG, 0, final)
    spread_relay(OUT_AG, 1, final)
    stores = []
    for g in range(groups):
        copy = finish(g)
        copy.start()
        stores.append(copy)
    for copy in stores:
        copy.wait()


def on_device(
    token_ids, prompt_lengths, cache_codes, cache_scales, embedding, norm_gain,
    query_weight, key_value_weight, output_weight,
):
    nm, nd = lax.axis_size("mp"), lax.axis_size("dp")
    vocab, width = embedding.shape
    rows, span = cache_codes.shape[:2]
    kvh = nm // 2
    nz, nq = nm // 2, nd // 2
    padded = -(-vocab // 512) * 512
    tokens = nd * NEW

    hbm = pl.BlockSpec(memory_space=pltpu.HBM)
    V = pltpu.VMEM
    out = pl.pallas_call(
        functools.partial(layer_kernel, nd, nm, width),
        out_shape=jax.ShapeDtypeStruct((nd, rows, NEW, width), BF16),
        in_specs=[hbm] * 9,
        out_specs=pl.BlockSpec(memory_space=pl.ANY),
        scratch_shapes=[
            V((padded, width), BF16),
            V((tokens, padded), BF16),
            V((tokens, 128), jnp.int32),
            V((rows, kvh, span, 2, HEAD), BF16),
            V((2 * max(span, width), HEAD), F32),
            V((rows, kvh, span, HEAD), BF16),
            V((rows, kvh, HEAD, span), BF16),
            V(query_weight.shape, BF16),
            V((width, 2, HEAD), BF16),
            V((width, HEAD), BF16),
            V(output_weight.shape, BF16),
            V((rows, nd, NEW, width), BF16),
            V((rows, nz, NEW, width), BF16),
            V((rows, nz, NEW, width), BF16),
            V((rows, nz - 1, NEW, width), BF16),
            V((rows, nm, NEW, width), BF16),
            V((rows, 2, nq, 11, 8, 128), F32),
            V((rows, nq, 11, 8, 128), F32),
            V((rows, nq, 11, 8, 128), F32),
            V((rows, nq - 1, 11, 8, 128), F32),
            V((rows, nm, 4, NEW, HEAD), BF16),
            V((rows, 2, NEW, HEAD), BF16),
            V((rows, nm, 64, 128), BF16),
            V((rows, nz, 64, 128), BF16),
            V((rows, nz, 64, 128), BF16),
            V((rows, nz - 1, 64, 128), BF16),
            V((rows, nm, 2, 128), F32),
            V((rows, nz, 2, 128), F32),
            V((rows, nz, 2, 128), F32),
            V((rows, nz - 1, 2, 128), F32),
            V((rows, nd, 4, NEW, HEAD), BF16),
            V((rows, nd, NEW, width), BF16),
            V((rows, nz, NEW, width), BF16),
            V((rows, nz, NEW, width), BF16),
            V((rows, nz - 1, NEW, width), BF16),
            V((rows, nm, NEW, width), BF16),
            pltpu.SMEM(prompt_lengths.shape, jnp.int32),
            V((NEW, rows * nd), jnp.int32),
            V(norm_gain.shape, BF16),
            V(cache_scales.shape, BF16),
            pltpu.SemaphoreType.DMA((3, rows, max(nm, nd) - 1)),
            pltpu.SemaphoreType.DMA((11, rows, max(nm, nd) - 1)),
            pltpu.SemaphoreType.DMA((11 + rows * kvh,)),
            pltpu.SemaphoreType.DMA((rows,)),
        ],
        compiler_params=pltpu.CompilerParams(
            collective_id=0, has_side_effects=True, vmem_limit_bytes=56 * 2**20
        ),
    )(
        prompt_lengths, token_ids.T, norm_gain, cache_scales,
        cache_codes, embedding, query_weight, key_value_weight, output_weight,
    )
    return out.reshape(nd * rows, NEW, width)


def solution(mesh):
    return jax.shard_map(
        on_device,
        mesh=mesh,
        in_specs=(
            P(),
            P(),
            P("dp", "mp", None, None),
            P("dp", "mp", None, None),
            P("mp", "dp"),
            P("dp"),
            P("dp", "mp"),
            P("dp", None, None),
            P("mp", "dp"),
        ),
        out_specs=P(None, None, "dp"),
        check_vma=False,
    )
```

```python
import functools

import jax
import jax.numpy as jnp
from jax import lax
from jax.experimental import pallas as pl
from jax.experimental.pallas import tpu as pltpu
from jax.sharding import PartitionSpec as P

HEAD = 128
FACTOR_GROUP = 128
NEW = 16
ROPE_BASE = 500000.0
EPSILON = 1e-05
LOWEST = -1e30
MESH = pl.DeviceIdType.MESH
BF16 = jnp.bfloat16
F32 = jnp.float32

EMB_RS, EMB_AG, CORE_RS, QKV_RS, QKV_AG, KV_SWAP, MIX_RS, STAT_RS, MIX_AG, OUT_RS, OUT_AG = range(11)
SENDERS = {CORE_RS: 1, KV_SWAP: 1, STAT_RS: 2}


def dot(a, b):
    return jnp.dot(a, b, preferred_element_type=F32)


def dot_last(a, b):
    return lax.dot_general(a, b, (((1,), (1,)), ((), ())), preferred_element_type=F32)


def layer_kernel(
    nd, nm, width,
    lens_hbm, ids_hbm, gain_hbm, scales_hbm, codes_hbm, emb_hbm, wq_hbm, wkv_hbm, wo_hbm,
    out_hbm,
    emb, onehot, idsb, codes, wide, keys, valuesT, wq, wkv_in, wkv, wo,
    look, look_x, look_pair, look_in, embedded, part, part_core, part_sum, part_in, heads, fresh,
    mix, mix_x, mix_pair, mix_in, stat, stat_x, stat_pair, stat_in, mixed, outp, outp_x, outp_pair, outp_in, final,
    lens_ref, ids_ref, gain_ref, scales_ref,
    send_sem, recv_sem, load_sem, store_sem,
):
    d, m = lax.axis_index("dp"), lax.axis_index("mp")
    groups = 2
    vocab = emb_hbm.shape[0]
    tokens = nd * NEW
    kvh = nm // 2
    nz, nq = nm // 2, nd // 2
    column, z = m // nz, lax.rem(m, nz)
    chip, core = d // 2, lax.rem(d, 2)
    span = codes_hbm.shape[1]
    blocks = span // FACTOR_GROUP
    lane = lambda shape: lax.broadcasted_iota(jnp.int32, shape, len(shape) - 1)

    along_z = lambda i: (d, column * nz + lax.rem(z + i, nz))
    across = (d, (1 - column) * nz + z)
    along_dp = lambda i: (lax.rem(d + i, nd), m)
    along_chips = lambda i: (2 * lax.rem(chip + i, nq) + core, m)
    other_core = (2 * chip + 1 - core, m)
    kv_partner = (d, 2 * (m // 2) + 1 - lax.rem(m, 2))

    barrier = pltpu.get_barrier_semaphore()
    pl.semaphore_signal(barrier, inc=1, device_id=across, device_id_type=MESH)
    for along, n in ((along_z, nz), (along_dp, nd)):
        def hello(i, c, along=along):
            pl.semaphore_signal(barrier, inc=1, device_id=along(i), device_id_type=MESH)
            return c
        lax.fori_loop(1, n, hello, 0)

    n_loads = 7 + groups * kvh
    small = [
        pltpu.make_async_copy(src, dst, load_sem.at[n_loads + i])
        for i, (src, dst) in enumerate(
            ((ids_hbm, ids_ref), (lens_hbm, lens_ref), (gain_hbm, gain_ref), (scales_hbm, scales_ref))
        )
    ]
    chunk = vocab // 4
    loads = [
        pltpu.make_async_copy(
            emb_hbm.at[pl.ds(c * chunk, chunk)], emb.at[pl.ds(c * chunk, chunk)], load_sem.at[c]
        )
        for c in range(4)
    ]
    loads.append(pltpu.make_async_copy(wq_hbm, wq, load_sem.at[4]))
    loads.append(pltpu.make_async_copy(wo_hbm, wo, load_sem.at[5]))
    loads.append(
        pltpu.make_async_copy(
            wkv_hbm.at[:, :, pl.ds(pl.multiple_of((m // 2) * HEAD, HEAD), HEAD)], wkv_in, load_sem.at[6]
        )
    )
    code_loads = [
        pltpu.make_async_copy(
            codes_hbm.at[g, :, :, pl.ds(k * HEAD, HEAD)], codes.at[g, k], load_sem.at[7 + g * kvh + k]
        )
        for g in range(groups)
        for k in range(kvh)
    ]
    for copy in small + loads + code_loads:
        copy.start()

    def remote(ph, g, k, src, dst, device):
        return pltpu.make_async_remote_copy(
            src_ref=src, dst_ref=dst,
            send_sem=send_sem.at[SENDERS.get(ph, 0), g, k], recv_sem=recv_sem.at[ph, g, k],
            device_id=device, device_id_type=MESH,
        )

    def loop(lo, hi, f):
        def body(i, c):
            f(i)
            return c
        lax.fori_loop(lo, hi, body, 0)

    def order(t):
        return nz // 2 + ((t + 1) // 2) * (1 - 2 * lax.rem(t, 2))

    def scatter_copy(ph, g, along, src, dst, dest, i):
        return remote(ph, g, i - 1, src.at[g, dest], dst.at[g, i - 1], along(i))

    def scatter_start(ph, g, along, src, dst, me, n):
        loop(1, n, lambda i: scatter_copy(ph, g, along, src, dst, lax.rem(me + i, n), i).start())

    def scatter_wait(ph, g, along, src, dst, me, n):
        loop(1, n, lambda i: scatter_copy(ph, g, along, src, dst, lax.rem(me + i, n), i).wait())

    def gather_start(ph, g, buf):
        loop(1, nd, lambda i: remote(ph, g, i - 1, buf.at[g, d], buf.at[g, d], along_dp(i)).start())

    def gather_wait(ph, g, buf):
        def go(i):
            remote(ph, g, i - 1, buf.at[g, d], buf.at[g, d], along_dp(i)).wait_send()
            at = lax.rem(d + nd - i, nd)
            remote(ph, g, i - 1, buf.at[g, at], buf.at[g, at], along_dp(i)).wait_recv()
        loop(1, nd, go)

    def z_copy(ph, g, buf, i, at):
        return remote(ph, g, i - 1, buf.at[g, at], buf.at[g, at], along_z(i))

    def x_copy(ph, g, buf, i, at):
        return remote(ph, g, nz - 1 + i, buf.at[g, at], buf.at[g, at], across)

    def behind(i):
        return lax.rem(z + nz - i, nz)

    def spread_start(ph, g, buf):
        loop(0, nz - 1, lambda t: z_copy(ph, g, buf, order(nz - 2 - t), m).start())
        x_copy(ph, g, buf, 0, m).start()

    def spread_relay(ph, g, buf):
        def relay(t):
            i = order(nz - 2 - t)
            at = column * nz + behind(i)
            z_copy(ph, g, buf, i, at).wait_recv()
            x_copy(ph, g, buf, i, at).start()
        loop(0, nz - 1, relay)

    def spread_wait(ph, g, buf):
        loop(1, nz, lambda i: z_copy(ph, g, buf, i, m).wait_send())
        def done(i):
            x_copy(ph, g, buf, i, column * nz + behind(i)).wait_send()
            x_copy(ph, g, buf, i, (1 - column) * nz + behind(i)).wait_recv()
        loop(0, nz, done)

    def ahead(i):
        return lax.rem(z + i, nz)

    def fold_x(ph, g, src, xin, i):
        return remote(ph, g, nz - 1 + i, src.at[g, (1 - column) * nz + ahead(i)], xin.at[g, i], across)

    def fold_z(ph, g, pair, zin, i):
        return remote(ph, g, i - 1, pair.at[g, i], zin.at[g, i - 1], along_z(i))

    def fold_start(ph, g, src, xin, zin):
        loop(0, nz - 1, lambda t: fold_x(ph, g, src, xin, order(t)).start())
        fold_x(ph, g, src, xin, 0).start()

    def fold_relay(ph, g, src, xin, pair, zin):
        def relay(t):
            i = order(t)
            fold_x(ph, g, src, xin, i).wait()
            pair[g, i] = (src[g, column * nz + ahead(i)].astype(F32) + xin[g, i].astype(F32)).astype(BF16)
            fold_z(ph, g, pair, zin, i).start()
        loop(0, nz - 1, relay)

    def fold_wait(ph, g, src, xin, pair, zin):
        total = src[g, m].astype(F32)
        fold_x(ph, g, src, xin, 0).wait()
        total = total + xin[g, 0].astype(F32)
        loop(1, nz, lambda i: fold_z(ph, g, pair, zin, i).wait())
        for i in range(nz - 1):
            total = total + zin[g, i].astype(F32)
        return total.astype(BF16)

    padded = emb.shape[0]
    if padded > vocab:
        emb[pl.ds(vocab, padded - vocab), :] = jnp.zeros((padded - vocab, emb.shape[1]), BF16)
    base = m * vocab

    def lookup(g):
        for j in range(nd):
            r = 2 * j + g
            idsb[pl.ds(j * NEW, NEW), :] = jnp.broadcast_to(ids_ref[:, r : r + 1] - base, (NEW, 128))

        def build(c, carry):
            for s in range(4):
                at = pl.multiple_of((c * 4 + s) * 128, 128)
                hit = idsb[...] - at == lane((tokens, 128))
                onehot[:, pl.ds(at, 128)] = jnp.where(hit, 1.0, 0.0).astype(BF16)
            return carry
        lax.fori_loop(0, padded // 512, build, 0)

    def look_dot(g):
        look[g] = dot(onehot[...], emb[...]).astype(BF16).reshape(nd, NEW, width)

    small[0].wait()
    lookup(0)
    for c in range(4):
        loads[c].wait()
    look_dot(0)
    pl.semaphore_wait(barrier, nd + nz - 1)
    fold_start(EMB_RS, 0, look, look_x, look_in)
    lookup(1)
    look_dot(1)
    fold_start(EMB_RS, 1, look, look_x, look_in)

    def widen(g):
        def one(k, carry):
            wide[pl.ds(0, 2 * span), :] = codes[g, k].reshape(2 * span, HEAD).astype(F32)
            for b in range(blocks):
                sc = scales_ref[g, b, :, pl.ds(pl.multiple_of(k * HEAD, HEAD), HEAD)].astype(F32)
                rows = pl.ds(b * FACTOR_GROUP, FACTOR_GROUP)
                kk = wide[pl.ds(2 * b * FACTOR_GROUP, FACTOR_GROUP, 2), :] * sc[0:1]
                vv = wide[pl.ds(2 * b * FACTOR_GROUP + 1, FACTOR_GROUP, 2), :] * sc[1:2]
                keys[g, k, rows, :] = kk.astype(BF16)
                valuesT[g, k, :, rows] = vv.T.astype(BF16)
            return carry
        lax.fori_loop(0, kvh, one, 0)

    def emb_sum(g):
        embedded[g, m] = fold_wait(EMB_RS, g, look, look_x, look_pair, look_in)
        spread_start(EMB_AG, g, embedded)

    for copy in small[1:] + code_loads[:kvh]:
        copy.wait()
    widen(0)
    def relays(f, *args):
        return lambda g: f(args[0], g, *args[1:])
    def staged(relay, stage):
        for f in (relay, stage):
            for g in range(groups):
                f(g)
    staged(relays(fold_relay, EMB_RS, look, look_x, look_pair, look_in), emb_sum)
    for copy in code_loads[kvh:]:
        copy.wait()
    widen(1)
    for copy in loads[4:]:
        copy.wait()
    wide[pl.ds(0, 2 * width), :] = wkv_in[...].reshape(2 * width, HEAD).astype(F32)
    odd = lax.rem(m, 2)
    wkv[...] = wide[pl.ds(odd, width, 2), :].astype(BF16)

    half_lane = lax.rem(lane((NEW, HEAD)), HEAD // 2)
    exponent = half_lane.astype(F32) * (2.0 / HEAD)
    rates = jnp.exp(-jnp.log(jnp.full((NEW, HEAD), ROPE_BASE, F32)) * exponent)
    steps = lax.broadcasted_iota(jnp.int32, (NEW, HEAD), 0)
    sign = jnp.where(lane((NEW, HEAD)) < HEAD // 2, -1.0, 1.0)
    tables = []
    for g in range(groups):
        angles = (lens_ref[2 * d + g] + steps).astype(F32) * rates
        tables.append((jnp.cos(angles), jnp.sin(angles) * sign))

    def project(g):
        spread_wait(EMB_AG, g, embedded)
        x = embedded[g].reshape(tokens, width).astype(F32)
        scaled = (x * gain_ref[...].astype(F32).reshape(1, width)).astype(BF16)
        square = x * x
        s = square[:, 0:128]
        for c in range(1, width // 128):
            s = s + square[:, c * 128 : (c + 1) * 128]
        s = s.reshape(nd, 2, 8, 128)
        a = s[:, 0].reshape(nd * 8, 128)
        b = s[:, 1].reshape(nd * 8, 128)
        a = a + pltpu.roll(a, 64, 1)
        b = b + pltpu.roll(b, 64, 1)
        s = jnp.where(lane(a.shape) < 64, a, b).reshape(nq, 2, 8, 128)
        q = dot(scaled, wq[...])
        kv = dot(scaled, wkv[...]).reshape(nq, 2, 2, 8, 128)
        q = [q[:, c * HEAD : (c + 1) * HEAD].reshape(nq, 2, 2, 8, 128) for c in range(4)] + [kv]
        for e in range(2):
            for c in range(5):
                part[g, e, :, 2 * c : 2 * c + 2] = q[c][:, e]
            part[g, e, :, 10] = s[:, e]
        core_copy(g).start()

    def core_copy(g):
        return remote(CORE_RS, g, 0, part.at[g, 1 - core], part_core.at[g], other_core)

    def join_cores(g):
        core_copy(g).wait()
        part_sum[g] = part[g, core] + part_core[g]
        scatter_start(QKV_RS, g, along_chips, part_sum, part_in, chip, nq)

    def kv_copy(g, at):
        return remote(KV_SWAP, g, 1, fresh.at[g, at], fresh.at[g, at], kv_partner)

    def rotate_heads(g):
        scatter_wait(QKV_RS, g, along_chips, part_sum, part_in, chip, nq)
        total = part_sum[g, chip]
        for i in range(nq - 1):
            total = total + part_in[g, i]
        sq = total[10]
        low = lane((8, 128)) < 64
        sums = jnp.concatenate(
            [
                jnp.sum(jnp.where(low, sq, 0.0), axis=1, keepdims=True),
                jnp.sum(jnp.where(low, 0.0, sq), axis=1, keepdims=True),
            ],
            axis=0,
        )
        inverse = lax.rsqrt(sums / (nd * width) + EPSILON)
        cosine, sine = tables[g]
        for c in range(5):
            v = total[2 * c : 2 * c + 2].reshape(NEW, HEAD) * inverse
            turned = v * cosine + pltpu.roll(v, 64, 1) * sine
            if c < 4:
                heads[g, m, c] = turned.astype(BF16)
            else:
                fresh[g, odd] = jnp.where(odd == 1, v, turned).astype(BF16)
        spread_start(QKV_AG, g, heads)
        kv_copy(g, odd).start()

    factor = HEAD ** (-0.5)
    half = lane((64, 128)) < 64
    half2 = lane((2, 128)) < 64

    def attend(g):
        spread_wait(QKV_AG, g, heads)
        live = lens_ref[2 * d + g] - m * span
        allowed = lax.broadcasted_iota(jnp.int32, (span, 128), 0) < live

        def one(k, carry):
            q = heads[g, pl.ds(2 * k, 2)].reshape(128, HEAD)
            s = jnp.where(allowed, dot_last(keys[g, k], q) * factor, -jnp.inf)
            top = jnp.maximum(jnp.max(s, axis=0, keepdims=True), LOWEST)
            p = jnp.exp(s - top)
            st = jnp.concatenate([top, jnp.sum(p, axis=0, keepdims=True)], axis=0)
            o = dot(valuesT[g, k], p.astype(BF16))
            lo, hi = o[0:64], o[64:128]
            mix[g, 2 * k] = jnp.where(half, lo, pltpu.roll(hi, 64, 1)).astype(BF16)
            mix[g, 2 * k + 1] = jnp.where(half, pltpu.roll(lo, 64, 1), hi).astype(BF16)
            turned = pltpu.roll(st, 64, 1)
            stat[g, 2 * k] = jnp.where(half2, st, turned)
            stat[g, 2 * k + 1] = jnp.where(half2, turned, st)
            return carry
        lax.fori_loop(0, kvh, one, 0, unroll=True)
        def go(i):
            merge_x(g, i, MIX_RS).start()
            merge_x(g, i, STAT_RS).start()
        loop(0, nz - 1, lambda t: go(order(t)))
        go(0)

    def merge_x(g, i, ph):
        src, dst = (mix, mix_x) if ph == MIX_RS else (stat, stat_x)
        return fold_x(ph, g, src, dst, i)

    def merge_z(g, i, ph):
        src, dst = (mix_pair, mix_in) if ph == MIX_RS else (stat_pair, stat_in)
        return fold_z(ph, g, src, dst, i)

    def merge(g, i):
        merge_x(g, i, STAT_RS).wait()
        merge_x(g, i, MIX_RS).wait()
        at = column * nz + ahead(i)
        a, b = stat[g, at], stat_x[g, i]
        top = jnp.maximum(a[0:1], b[0:1])
        wa, wb = jnp.exp(a[0:1] - top), jnp.exp(b[0:1] - top)
        stat_pair[g, i] = jnp.concatenate([top, wa * a[1:2] + wb * b[1:2]], axis=0)
        mix_pair[g, i] = (wa * mix[g, at].astype(F32) + wb * mix_x[g, i].astype(F32)).astype(BF16)

    def merge_relay(g):
        def relay(t):
            i = order(t)
            merge(g, i)
            merge_z(g, i, MIX_RS).start()
            merge_z(g, i, STAT_RS).start()
        loop(0, nz - 1, relay)
        merge(g, 0)

    def fresh_part(g):
        kv_copy(g, odd).wait_send()
        kv_copy(g, 1 - odd).wait_recv()
        q = heads[g, m].reshape(64, HEAD)
        q = jnp.concatenate([q, q], axis=0)
        s = dot_last(fresh[g, 0], q) * factor
        step = lax.rem(lane((NEW, 128)), NEW)
        s = jnp.where(lax.broadcasted_iota(jnp.int32, (NEW, 128), 0) <= step, s, -jnp.inf)
        top = jnp.max(s, axis=0, keepdims=True)
        p = jnp.exp(s - top)
        o = dot(fresh[g, 1].astype(F32).T.astype(BF16), p.astype(BF16))
        return top, jnp.sum(p, axis=0, keepdims=True), jnp.where(half, o[0:64], o[64:128])

    def mix_heads(g):
        top_f, sum_f, o_f = fresh_part(g)
        def done(i):
            merge_z(g, i, STAT_RS).wait()
            merge_z(g, i, MIX_RS).wait()
        loop(1, nz, done)
        stats = [stat_pair[g, 0]] + [stat_in[g, i] for i in range(nz - 1)]
        largest = top_f
        for st in stats:
            largest = jnp.maximum(largest, st[0:1])
        w = jnp.exp(top_f - largest)
        total = sum_f * w
        acc = o_f * w
        for i, st in enumerate(stats):
            w = jnp.exp(st[0:1] - largest)
            total = total + w * st[1:2]
            o = mix_pair[g, 0] if i == 0 else mix_in[g, i - 1]
            acc = acc + w * o.astype(F32)
        acc = acc / total
        full = jnp.concatenate([acc, pltpu.roll(acc, 64, 1)], axis=0)
        mixed[g, d] = full.T[0:64].astype(BF16).reshape(4, NEW, HEAD)
        gather_start(MIX_AG, g, mixed)

    def out_project(g):
        gather_wait(MIX_AG, g, mixed)
        a = jnp.concatenate([mixed[g, :, h].reshape(tokens, HEAD) for h in range(4)], axis=1)
        outp[g] = dot(a, wo[...]).astype(BF16).reshape(nd, NEW, width)
        fold_start(OUT_RS, g, outp, outp_x, outp_in)

    def out_sum(g):
        final[g, m] = fold_wait(OUT_RS, g, outp, outp_x, outp_pair, outp_in)
        spread_start(OUT_AG, g, final)

    def finish(g):
        spread_wait(OUT_AG, g, final)
        return pltpu.make_async_copy(final.at[g], out_hbm.at[:, g], store_sem.at[g])

    nothing = lambda g: None
    staged(relays(spread_relay, EMB_AG, embedded), project)
    staged(nothing, join_cores)
    staged(nothing, rotate_heads)
    staged(relays(spread_relay, QKV_AG, heads), attend)
    staged(merge_relay, mix_heads)
    staged(nothing, out_project)
    staged(relays(fold_relay, OUT_RS, outp, outp_x, outp_pair, outp_in), out_sum)
    spread_relay(OUT_AG, 0, final)
    spread_relay(OUT_AG, 1, final)
    stores = []
    for g in range(groups):
        copy = finish(g)
        copy.start()
        stores.append(copy)
    for copy in stores:
        copy.wait()


def on_device(
    token_ids, prompt_lengths, cache_codes, cache_scales, embedding, norm_gain,
    query_weight, key_value_weight, output_weight,
):
    nm, nd = lax.axis_size("mp"), lax.axis_size("dp")
    vocab, width = embedding.shape
    rows, span = cache_codes.shape[:2]
    kvh = nm // 2
    nz, nq = nm // 2, nd // 2
    padded = -(-vocab // 512) * 512
    tokens = nd * NEW

    hbm = pl.BlockSpec(memory_space=pltpu.HBM)
    V = pltpu.VMEM
    out = pl.pallas_call(
        functools.partial(layer_kernel, nd, nm, width),
        out_shape=jax.ShapeDtypeStruct((nd, rows, NEW, width), BF16),
        in_specs=[hbm] * 9,
        out_specs=pl.BlockSpec(memory_space=pl.ANY),
        scratch_shapes=[
            V((padded, width), BF16),
            V((tokens, padded), BF16),
            V((tokens, 128), jnp.int32),
            V((rows, kvh, span, 2, HEAD), BF16),
            V((2 * max(span, width), HEAD), F32),
            V((rows, kvh, span, HEAD), BF16),
            V((rows, kvh, HEAD, span), BF16),
            V(query_weight.shape, BF16),
            V((width, 2, HEAD), BF16),
            V((width, HEAD), BF16),
            V(output_weight.shape, BF16),
            V((rows, nd, NEW, width), BF16),
            V((rows, nz, NEW, width), BF16),
            V((rows, nz, NEW, width), BF16),
            V((rows, nz - 1, NEW, width), BF16),
            V((rows, nm, NEW, width), BF16),
            V((rows, 2, nq, 11, 8, 128), F32),
            V((rows, nq, 11, 8, 128), F32),
            V((rows, nq, 11, 8, 128), F32),
            V((rows, nq - 1, 11, 8, 128), F32),
            V((rows, nm, 4, NEW, HEAD), BF16),
            V((rows, 2, NEW, HEAD), BF16),
            V((rows, nm, 64, 128), BF16),
            V((rows, nz, 64, 128), BF16),
            V((rows, nz, 64, 128), BF16),
            V((rows, nz - 1, 64, 128), BF16),
            V((rows, nm, 2, 128), F32),
            V((rows, nz, 2, 128), F32),
            V((rows, nz, 2, 128), F32),
            V((rows, nz - 1, 2, 128), F32),
            V((rows, nd, 4, NEW, HEAD), BF16),
            V((rows, nd, NEW, width), BF16),
            V((rows, nz, NEW, width), BF16),
            V((rows, nz, NEW, width), BF16),
            V((rows, nz - 1, NEW, width), BF16),
            V((rows, nm, NEW, width), BF16),
            pltpu.SMEM(prompt_lengths.shape, jnp.int32),
            V((NEW, rows * nd), jnp.int32),
            V(norm_gain.shape, BF16),
            V(cache_scales.shape, BF16),
            pltpu.SemaphoreType.DMA((3, rows, max(nm, nd) - 1)),
            pltpu.SemaphoreType.DMA((11, rows, max(nm, nd) - 1)),
            pltpu.SemaphoreType.DMA((11 + rows * kvh,)),
            pltpu.SemaphoreType.DMA((rows,)),
        ],
        compiler_params=pltpu.CompilerParams(
            collective_id=0, has_side_effects=True, vmem_limit_bytes=56 * 2**20
        ),
    )(
        prompt_lengths, token_ids.T, norm_gain, cache_scales,
        cache_codes, embedding, query_weight, key_value_weight, output_weight,
    )
    return out.reshape(nd * rows, NEW, width)


def solution(mesh):
    return jax.shard_map(
        on_device,
        mesh=mesh,
        in_specs=(
            P(),
            P(),
            P("dp", "mp", None, None),
            P("dp", "mp", None, None),
            P("mp", "dp"),
            P("dp"),
            P("dp", "mp"),
            P("dp", None, None),
            P("mp", "dp"),
        ),
        out_specs=P(None, None, "dp"),
        check_vma=False,
    )
```
